128 devices in a mesh: row: 8 (over z, core), col: 16 (over y, x).
Axes of the slice: x: 4, y: 4, z: 4, core: 2. Of those that a mesh axis runs over, the one named last changes fastest.
Arguments:
- features: bfloat16 [131072, 256], P(('row', 'col')), may hold values from -6 to 6
- tile_values: bfloat16 [8, 16, 256, 128, 128], P('row', 'col'), may hold values from -0.09375 to 0.09375
- tile_rows: int32 [8, 16, 256], P('row', 'col'), may hold values from 0 to 127, as said below
- tile_cols: int32 [8, 16, 256], P('row', 'col'), may hold values from 0 to 63, as said below
- tile_count: int32 [8, 16], P('row', 'col'), may hold values from 64 to 256, as said below
- w_first: bfloat16 [256, 256], replicated, may hold values from -0.375 to 0.375
- w_second: bfloat16 [256, 256], replicated, may hold values from -0.375 to 0.375
Outputs:
- output: bfloat16 [131072, 256], P(('row', 'col'))
The draws below stay inside these ranges and needn't reach their ends.
Inputs may be any that keep to these rules, and one draw needn't show every extreme that they name: `tile_rows`: in each block the slots name distinct tiles; the first tile_count slots are ordered by tile column, then tile row; later slots are padding. `tile_cols`: as for tile_rows. `tile_count`: some block uses all 256 slots.
All inputs are finite; a program needn't handle non-finite values.
Results may differ from the reference program's by a relative error of at most 0.024.
Values may be sent and summed in bfloat16 or wider, within the bound.
A program may use at most 192 MiB of HBM per device.

```python
import jax
import jax.numpy as jnp
from jax import lax

F = 256
TILE = 128
NODE_DEV = 1024
TILES = 256
TILE_ROWS = 128
TILE_COLS = 64
NODES = 131072
N_ROW = 8
N_COL = 16


def tile_layout(key):
    device_total = N_ROW * N_COL
    slots_total = TILE_ROWS * TILE_COLS
    layout_key = jax.random.fold_in(key, 4242)
    heaviest = jax.random.randint(jax.random.fold_in(layout_key, 1), (), 0, device_total)
    others = jax.random.randint(jax.random.fold_in(layout_key, 2), (device_total,), TILES // 4, TILES + 1)
    counts = jnp.where(jnp.arange(device_total, dtype=jnp.int32) == heaviest, TILES, others).astype(jnp.int32)

    def one_block(device, filled):
        chosen = jax.random.permutation(jax.random.fold_in(layout_key, 100 + device), slots_total)[:TILES]
        slot_ids = jnp.arange(TILES, dtype=jnp.int32)
        marked = jnp.where(slot_ids < filled, chosen, chosen + slots_total).astype(jnp.int32)
        ordered = jnp.sort(marked)
        flat_index = ordered % slots_total
        return (flat_index % TILE_ROWS, flat_index // TILE_ROWS)
    row_ids, col_ids = jax.vmap(one_block)(jnp.arange(device_total, dtype=jnp.int32), counts)
    return (row_ids.reshape(N_ROW, N_COL, TILES).astype(jnp.int32), col_ids.reshape(N_ROW, N_COL, TILES).astype(jnp.int32), counts.reshape(N_ROW, N_COL))


def draw_tile_rows(key, part):
    return tile_layout(key)[0]


def draw_tile_cols(key, part):
    return tile_layout(key)[1]


def draw_tile_count(key, part):
    return tile_layout(key)[2]


def block_levels(rng, shape, pieces, least, largest):
    def one(axis_at, parts):
        draws = jax.random.uniform(jax.random.fold_in(jax.random.fold_in(rng, 6), axis_at), (parts,), jnp.float32, least / len(pieces), largest / len(pieces))
        return jnp.repeat(jnp.exp(draws), shape[axis_at] // parts).reshape((-1,) + (1,) * (len(shape) - axis_at - 1))

    factor_of = one(*pieces[0])
    for cut in pieces[1:]:
        factor_of = factor_of * one(*cut)
    return factor_of


def centred(own_key, extent, width, most, cuts=(), held_as=jnp.bfloat16):
    drawn = jax.random.normal(own_key, extent, jnp.float32) * width
    if len(cuts) > 0:
        drawn = block_levels(own_key, extent, cuts, -0.22, 0.18) * drawn
    return jnp.clip(drawn, min=-most, max=most).astype(held_as)


def setup_inputs(seed: int = 0) -> dict:
    key_of = jax.random.split(jax.random.key(seed), 8)
    return {
        "features": centred(key_of[0], (NODES, F), 1.0, 6.0, ((0, 128),)),
        "tile_values": centred(key_of[1], (N_ROW, N_COL, TILES, TILE, TILE), (TILES * TILE * TILE // NODE_DEV) ** -0.5, 0.09375, ((0, 8), (1, 16))),
        "tile_rows": draw_tile_rows(jax.random.fold_in(key_of[7], 71), 0),
        "tile_cols": draw_tile_cols(jax.random.fold_in(key_of[7], 71), 0),
        "tile_count": draw_tile_count(jax.random.fold_in(key_of[7], 71), 0),
        "w_first": centred(key_of[5], (F, F), F ** -0.5, 0.375),
        "w_second": centred(key_of[6], (F, F), F ** -0.5, 0.375),
    }


def block_partial(values, row_ids, col_ids, filled, panel_tiles):
    active = (jnp.arange(TILES, dtype=jnp.int32) < filled).astype(jnp.float32)
    inputs = panel_tiles[col_ids].astype(jnp.float32)
    products = jnp.einsum("gij,gjf->gif", values.astype(jnp.float32), inputs) * active[:, None, None]
    return jax.ops.segment_sum(products, row_ids, num_segments=TILE_ROWS)


def aggregate(inputs_now, tile_values, tile_rows, tile_cols, tile_count):
    blocks = inputs_now.reshape(N_ROW, N_COL, NODE_DEV, F)

    def row_block(row_index):
        def add_col(running, col_index):
            panel_tiles = blocks[:, col_index].reshape(N_ROW * NODE_DEV // TILE, TILE, F)
            partial_value = block_partial(tile_values[row_index, col_index], tile_rows[row_index, col_index],
                                    tile_cols[row_index, col_index], tile_count[row_index, col_index], panel_tiles)
            rounded = lax.optimization_barrier(partial_value.astype(jnp.bfloat16))
            return running + rounded.astype(jnp.float32), None

        running, unused = lax.scan(add_col, jnp.zeros((TILE_ROWS, TILE, F), jnp.float32),
                                   jnp.arange(N_COL, dtype=jnp.int32))
        return running.astype(jnp.bfloat16)

    summed = lax.map(row_block, jnp.arange(N_ROW, dtype=jnp.int32))
    return summed.reshape(N_ROW * N_COL * NODE_DEV, F)


def reference(features, tile_values, tile_rows, tile_cols, tile_count, w_first, w_second):
    summed = aggregate(features, tile_values, tile_rows, tile_cols, tile_count)
    hidden = jax.nn.relu(jnp.dot(summed, w_first, preferred_element_type=jnp.float32)).astype(jnp.bfloat16)
    summed_two = aggregate(hidden, tile_values, tile_rows, tile_cols, tile_count)
    return jax.nn.relu(jnp.dot(summed_two, w_second, preferred_element_type=jnp.float32)).astype(jnp.bfloat16)
```

```python
import functools

import jax
import jax.numpy as jnp
from jax import lax
from jax.experimental import pallas as pl
from jax.experimental.pallas import tpu as pltpu
from jax.sharding import PartitionSpec as P

MESH = pl.DeviceIdType.MESH
F = 256
TILE = 128
SLOTS = 256
ROW_TILES = 128
COL_TILES = 64
NODES = 1024
PIECE = 256
SIDE = 4
OFFSETS = (2, 1, 3, 0)
FAR, RAW, MERGED = 0, 1, 2


def remote(src, dst, send, recv, row, col):
    return pltpu.make_async_remote_copy(
        src_ref=src, dst_ref=dst, send_sem=send, recv_sem=recv, device_id=(row, col), device_id_type=MESH
    )


def greet(partners):
    barrier = pltpu.get_barrier_semaphore()
    for row, col in partners:
        pl.semaphore_signal(barrier, inc=1, device_id=(row, col), device_id_type=MESH)
    pl.semaphore_wait(barrier, len(partners))


def gather_kernel(x_hbm, panel_hbm, held, send, recv, mate_send, mate_recv, local, out_sem):
    row, col = lax.axis_index("row"), lax.axis_index("col")
    z, core = row // 2, row % 2
    mate = z * 2 + 1 - core
    half = NODES // 2
    steps = ((z + 1) % SIDE * 2 + core, (z + 3) % SIDE * 2 + core)
    load = pltpu.make_async_copy(x_hbm, held.at[row], local)
    load.start()
    greet([(steps[0], col), (steps[1], col), (mate, col)])
    load.wait()

    def part(block, which):
        return held.at[block, pl.ds(which * half, half)]

    def hop(way, order, block, which):
        piece = part(block, which)
        return remote(piece, piece, send.at[way, order], recv.at[way, order], steps[way], col)

    def share(order, block, which):
        piece = part(block, which)
        return remote(piece, piece, mate_send.at[order], mate_recv.at[order], mate, col)

    def put(order, block, which):
        piece = part(block, which)
        return pltpu.make_async_copy(piece, panel_hbm.at[block, pl.ds(which * half, half)], out_sem.at[order])

    def at(distance, k):
        return (z + distance) % SIDE * 2 + k

    own = ((0, 0), (0, 1))
    first = ((3, 0), (1, 1))
    second = ((3, 1), (1, 0))
    last = ((2, 0), (2, 1))
    pieces = own + first + second + last
    started = []

    def begin(copy):
        copy.start()
        started.append(copy)

    for order in range(2):
        for way in range(2):
            begin(hop(way, order, row, way ^ order))
    for order in range(2):
        begin(share(order, row, order))
        begin(put(order, row, order))
    count = 2
    for order, group in enumerate((first, second, last)):
        for way in range(2):
            distance, which = group[way]
            block = at(distance, core)
            hop(way, order, block, which).wait_recv()
            if order == 0:
                begin(hop(way, 2, block, which))
            begin(share(count, block, which))
            begin(put(count, block, which))
            count += 1
    for order in range(8):
        distance, which = pieces[order]
        block = at(distance, 1 - core)
        share(order, block, which).wait_recv()
        begin(put(8 + order, block, which))
    for copy in started:
        if copy.is_remote:
            copy.wait_send()
        else:
            copy.wait()


def gather(x, number):
    return pl.pallas_call(
        gather_kernel,
        out_shape=jax.ShapeDtypeStruct((8, NODES, F), jnp.bfloat16),
        in_specs=[pl.BlockSpec(memory_space=pl.ANY)],
        out_specs=pl.BlockSpec(memory_space=pl.ANY),
        scratch_shapes=[
            pltpu.VMEM((8, NODES, F), jnp.bfloat16),
            pltpu.SemaphoreType.DMA((2, 3)),
            pltpu.SemaphoreType.DMA((2, 3)),
            pltpu.SemaphoreType.DMA((8,)),
            pltpu.SemaphoreType.DMA((8,)),
            pltpu.SemaphoreType.DMA,
            pltpu.SemaphoreType.DMA((16,)),
        ],
        compiler_params=pltpu.CompilerParams(collective_id=number, has_side_effects=True),
        name="gather",
    )(x)


UNROLL = 16
LOADS = 8


def tiles_kernel(rows, cols, count, values_hbm, panel_hbm, out_hbm, values, panel, total, staged, value_sem, panel_sem, out_sem):
    per_load = SLOTS // LOADS
    panel_copy = pltpu.make_async_copy(panel_hbm, panel, panel_sem)
    panel_copy.start()

    def load(g):
        window = pl.ds(g * per_load, per_load)
        return pltpu.make_async_copy(values_hbm.at[window], values.at[window], value_sem.at[g])

    for g in range(LOADS):
        load(g).start()

    @pl.loop(0, ROW_TILES + 1)
    def _(t):
        total[t] = jnp.zeros((TILE, F), jnp.float32)

    panel_copy.wait()
    filled = count[0]
    for g in range(LOADS):
        load(g).wait()

        @pl.loop(0, per_load // UNROLL)
        def _(step):
            base = g * per_load + step * UNROLL
            for u in range(UNROLL):
                slot = base + u
                product = jnp.dot(values[slot], panel[cols[slot]], preferred_element_type=jnp.float32)
                target = jnp.where(slot < filled, rows[slot], ROW_TILES)
                total[target] += product

    per_part = ROW_TILES // 16

    def store(part):
        return pltpu.make_async_copy(
            staged.at[part % 4], out_hbm.at[pl.ds(part * per_part, per_part)], out_sem.at[part % 4]
        )

    for part in range(16):
        if part >= 4:
            store(part - 4).wait()

        @pl.loop(0, per_part)
        def _(t):
            staged[part % 4, t] = total[part * per_part + t].astype(jnp.bfloat16)

        store(part).start()
    for part in range(12, 16):
        store(part).wait()


def tiles(rows, cols, count, values, panel):
    scalar = pl.BlockSpec(memory_space=pltpu.SMEM)
    array = pl.BlockSpec(memory_space=pl.ANY)
    return pl.pallas_call(
        tiles_kernel,
        out_shape=jax.ShapeDtypeStruct((ROW_TILES, TILE, F), jnp.bfloat16),
        in_specs=[scalar, scalar, scalar, array, array],
        out_specs=array,
        scratch_shapes=[
            pltpu.VMEM((SLOTS, TILE, TILE), jnp.bfloat16),
            pltpu.VMEM((COL_TILES, TILE, F), jnp.bfloat16),
            pltpu.VMEM((ROW_TILES + 1, TILE, F), jnp.float32),
            pltpu.VMEM((4, ROW_TILES // 16, TILE, F), jnp.bfloat16),
            pltpu.SemaphoreType.DMA((LOADS,)),
            pltpu.SemaphoreType.DMA,
            pltpu.SemaphoreType.DMA((4,)),
        ],
        compiler_params=pltpu.CompilerParams(vmem_limit_bytes=60 * 2**20),
        name="tiles",
    )(rows, cols, count, values, panel)


def add_up(target, terms):
    @pl.loop(0, PIECE // 64)
    def _(t):
        lines = pl.ds(t * 64, 64)
        total = terms[0][lines].astype(jnp.float32)
        for term in terms[1:]:
            total = total + term[lines].astype(jnp.float32)
        target[lines] = total.astype(target.dtype)


def reduce_kernel(
    part_hbm, w, out, near, own, got1, merged1, result, got2, merged2, summed,
    near_sem, own_sem, send1, recv1, send2, recv2,
):
    row, col = lax.axis_index("row"), lax.axis_index("col")
    y, x = col // SIDE, col % SIDE

    def place(half, first, second):
        return second * SIDE + first if half == 0 else first * SIDE + second

    def spot(half):
        return (x, y) if half == 0 else (y, x)

    def step(at, way):
        return (at + (1 if way == 0 else SIDE - 1)) % SIDE

    def piece(half, first, second, h):
        return part_hbm.at[place(half, first, second), 2 * half + h]

    def loads(half):
        first, second = spot(half)
        made = []
        for q in range(SIDE):
            there = (second + OFFSETS[q]) % SIDE
            for way in range(2):
                made.append(
                    pltpu.make_async_copy(
                        piece(half, step(first, way), there, way), near.at[half, way, q], near_sem.at[half, way, q]
                    )
                )
            for h in range(2):
                made.append(
                    pltpu.make_async_copy(piece(half, first, there, h), own.at[half, q, h], own_sem.at[half, q, h])
                )
        return made

    def hop1(half, way, kind, q):
        first, second = spot(half)
        there = (second + OFFSETS[q]) % SIDE
        if kind == FAR:
            src = piece(half, (first + 2) % SIDE, there, way)
        elif kind == RAW:
            src = piece(half, step(first, way), there, 1 - way)
        else:
            src = merged1.at[half, way, q]
        return remote(
            src, got1.at[half, way, kind, q], send1.at[half, way, kind, q], recv1.at[half, way, kind, q],
            row, place(half, step(first, way), second),
        )

    def hop2(half, way, kind):
        first, second = spot(half)
        if kind == FAR:
            src = result.at[half, 0, way]
        elif kind == RAW:
            src = result.at[half, 1 + way, 1 - way]
        else:
            src = merged2.at[half, way]
        return remote(
            src, got2.at[half, way, kind], send2.at[half, way, kind], recv2.at[half, way, kind],
            row, place(half, first, step(second, way)),
        )

    local = loads(0) + loads(1)
    for copy in local:
        copy.start()
    greet([(row, place(half, step(spot(half)[0], way), spot(half)[1])) for half in range(2) for way in range(2)])
    started = []

    def begin(copy):
        copy.start()
        started.append(copy)

    both = [(half, way) for half in range(2) for way in range(2)]
    for q in range(SIDE):
        for kind in (FAR, RAW):
            for half, way in both:
                begin(hop1(half, way, kind, q))
    for copy in local:
        copy.wait()
    for q in range(SIDE):
        for half, way in both:
            hop1(half, way, FAR, q).wait_recv()
            add_up(merged1.at[half, way, q], [near.at[half, way, q], got1.at[half, way, FAR, q]])
            begin(hop1(half, way, MERGED, q))
    for q in range(3):
        for half in range(2):
            for h in range(2):
                hop1(half, h, MERGED, q).wait_recv()
                hop1(half, 1 - h, RAW, q).wait_recv()
                add_up(
                    result.at[half, q, h],
                    [own.at[half, q, h], got1.at[half, h, MERGED, q], got1.at[half, 1 - h, RAW, q]],
                )
                if q == 0:
                    begin(hop2(half, h, FAR))
                elif h == 2 - q:
                    begin(hop2(half, q - 1, RAW))
    for half, way in both:
        hop2(half, way, FAR).wait_recv()
        add_up(merged2.at[half, way], [result.at[half, 1 + way, way], got2.at[half, way, FAR]])
        begin(hop2(half, way, MERGED))
    for half in range(2):
        for h in range(2):
            hop1(half, h, MERGED, 3).wait_recv()
            hop1(half, 1 - h, RAW, 3).wait_recv()
    for half in range(2):
        for h in range(2):
            hop2(half, h, MERGED).wait_recv()
            hop2(half, 1 - h, RAW).wait_recv()
            add_up(
                summed,
                [
                    own.at[half, 3, h], got1.at[half, h, MERGED, 3], got1.at[half, 1 - h, RAW, 3],
                    got2.at[half, h, MERGED], got2.at[half, 1 - h, RAW],
                ],
            )
            product = jnp.dot(summed[...], w[...], preferred_element_type=jnp.float32)
            out[pl.ds((2 * half + h) * PIECE, PIECE)] = jnp.maximum(product, 0.0).astype(jnp.bfloat16)
    for copy in started:
        copy.wait_send()


def reduce(part, w, number):
    block = (PIECE, F)
    dtype = jnp.bfloat16
    vmem = pl.BlockSpec(memory_space=pltpu.VMEM)
    return pl.pallas_call(
        reduce_kernel,
        out_shape=jax.ShapeDtypeStruct((NODES, F), dtype),
        in_specs=[pl.BlockSpec(memory_space=pl.ANY), vmem],
        out_specs=vmem,
        scratch_shapes=[
            pltpu.VMEM((2, 2, 4) + block, dtype),
            pltpu.VMEM((2, 4, 2) + block, dtype),
            pltpu.VMEM((2, 2, 3, 4) + block, dtype),
            pltpu.VMEM((2, 2, 4) + block, dtype),
            pltpu.VMEM((2, 3, 2) + block, dtype),
            pltpu.VMEM((2, 2, 3) + block, dtype),
            pltpu.VMEM((2, 2) + block, dtype),
            pltpu.VMEM(block, dtype),
            pltpu.SemaphoreType.DMA((2, 2, 4)),
            pltpu.SemaphoreType.DMA((2, 4, 2)),
            pltpu.SemaphoreType.DMA((2, 2, 3, 4)),
            pltpu.SemaphoreType.DMA((2, 2, 3, 4)),
            pltpu.SemaphoreType.DMA((2, 2, 3)),
            pltpu.SemaphoreType.DMA((2, 2, 3)),
        ],
        compiler_params=pltpu.CompilerParams(
            collective_id=number, has_side_effects=True, vmem_limit_bytes=60 * 2**20
        ),
        name="reduce",
    )(part, w)


def shards(features, tile_values, tile_rows, tile_cols, tile_count, w_first, w_second):
    rows, cols, count = tile_rows[0, 0], tile_cols[0, 0], tile_count[0]
    values = tile_values[0, 0]
    current = features
    for layer, weight in enumerate((w_first, w_second)):
        panel = gather(current, 2 * layer)
        part = tiles(rows, cols, count, values, panel.reshape(COL_TILES, TILE, F))
        current = reduce(part.reshape(16, 4, PIECE, F), weight, 2 * layer + 1)
    return current


def solution(mesh):
    return jax.shard_map(
        shards,
        mesh=mesh,
        in_specs=(
            P(("row", "col"), None),
            P("row", "col", None, None, None),
            P("row", "col", None),
            P("row", "col", None),
            P("row", "col"),
            P(),
            P(),
        ),
        out_specs=P(("row", "col"), None),
        check_vma=False,
    )
```

```python
import jax
import jax.numpy as jnp
from jax import lax
from jax.experimental import pallas as pl
from jax.experimental.pallas import tpu as pltpu
from jax.sharding import PartitionSpec as P

MESH = pl.DeviceIdType.MESH
F = 256
WIDE = 128
TILE = 128
SLOTS = 256
NODES = 1024
SIDE = 4
BLOCK_TILES = NODES // TILE
UNROLL = 32
FAR, RAW, MERGED = 0, 1, 2
BF16 = jnp.bfloat16

UNITS = (
    ((0, 1, 0, 512), (0, 1, 512, 512), (1, 1, 0, 256), (1, 1, 256, 256), (1, 1, 512, 256), (1, 1, 768, 256)),
    ((0, 1, 0, 1024), (1, 1, 0, 512), (1, 1, 512, 512)),
)
SPREADS = (
    ((0, 1, 0, 8), (0, 1, 0, 8)),
    ((0, 2, 0, 2), (0, 2, 2, 2), (0, 2, 4, 2), (0, 2, 6, 2)),
)


def remote(src, dst, send, recv, row, col):
    return pltpu.make_async_remote_copy(
        src_ref=src, dst_ref=dst, send_sem=send, recv_sem=recv, device_id=(row, col), device_id_type=MESH
    )


def await_bytes(sized, sem):
    pltpu.make_async_copy(sized, sized, sem).wait()


class Spread:
    def __init__(self, unit, panel, sems, row, col):
        self.f0, self.nf, self.t0, self.tiles = unit
        self.panel, self.row, self.col = panel, row, col
        self.send, self.recv, self.mate_send, self.mate_recv = sems
        self.z, self.core = row // 2, row % 2
        self.mate = self.z * 2 + 1 - self.core
        self.steps = ((self.z + 1) % SIDE * 2 + self.core, (self.z + 3) % SIDE * 2 + self.core)
        self.groups = (((3, 0), (1, 1)), ((3, 1), (1, 0)), ((2, 0), (2, 1)))

    def at(self, distance, core):
        return (self.z + distance) % SIDE * 2 + core

    def part(self, block, which):
        half = self.tiles // 2
        return self.panel.at[pl.ds(self.f0, self.nf), pl.ds(block * BLOCK_TILES + self.t0 + which * half, half)]

    def sized(self, tiles):
        return self.panel.at[pl.ds(self.f0, self.nf), pl.ds(0, tiles)]

    def hop(self, way, order, block, which):
        piece = self.part(block, which)
        remote(piece, piece, self.send, self.recv.at[order], self.steps[way], self.col).start()

    def share(self, block, which):
        piece = self.part(block, which)
        remote(piece, piece, self.mate_send, self.mate_recv, self.mate, self.col).start()

    def own(self):
        for order in range(2):
            for way in range(2):
                self.hop(way, order, self.row, way ^ order)
        for which in range(2):
            self.share(self.row, which)

    def onward(self, order):
        await_bytes(self.sized(self.tiles), self.recv.at[order])
        for way in range(2):
            distance, which = self.groups[order][way]
            block = self.at(distance, self.core)
            if order == 0:
                self.hop(way, 2, block, which)
            self.share(block, which)

    def finish(self):
        await_bytes(self.sized(4 * self.tiles), self.mate_recv)

    def drain(self):
        await_bytes(self.sized(3 * self.tiles), self.send)
        await_bytes(self.sized(4 * self.tiles), self.mate_send)


class Sum:
    def __init__(self, unit, part, got1, got2, sems, row, col):
        self.f0, self.nf, self.r0, self.rows = unit
        self.quarter = self.rows // 4
        self.part, self.got1, self.got2 = part, got1, got2
        self.send1, self.recv1, self.send2, self.recv2 = sems
        self.row = row
        self.y, self.x = col // SIDE, col % SIDE

    def spot(self, half):
        return (self.x, self.y) if half == 0 else (self.y, self.x)

    def step(self, at, way):
        return (at + (1 if way == 0 else SIDE - 1)) % SIDE

    def place(self, half, first, second):
        return second * SIDE + first if half == 0 else first * SIDE + second

    def lines(self, half, h):
        return pl.ds(self.r0 + (2 * half + h) * self.quarter, self.quarter)

    def group(self, half, first, h):
        halves = pl.ds(self.f0, self.nf)
        if half == 0:
            return self.part.at[halves, :, first, self.lines(half, h)]
        return self.part.at[halves, first, :, self.lines(half, h)]

    def single(self, half, second, h):
        halves = pl.ds(self.f0, self.nf)
        first = self.spot(half)[0]
        if half == 0:
            return self.part.at[halves, second, first, self.lines(half, h)]
        return self.part.at[halves, first, second, self.lines(half, h)]

    def hop1(self, half, way, kind):
        first, second = self.spot(half)
        if kind == FAR:
            src = self.group(half, (first + 2) % SIDE, way)
        elif kind == RAW:
            src = self.group(half, self.step(first, way), 1 - way)
        else:
            src = self.group(half, self.step(first, way), way)
        remote(
            src, self.got1.at[half, way, kind], self.send1, self.recv1.at[half, min(kind, 1)],
            self.row, self.place(half, self.step(first, way), second),
        ).start()

    def hop2(self, half, way, kind):
        first, second = self.spot(half)
        if kind == FAR:
            src = self.single(half, (second + 2) % SIDE, way)
        elif kind == RAW:
            src = self.single(half, self.step(second, way), 1 - way)
        else:
            src = self.single(half, self.step(second, way), way)
        remote(
            src, self.got2.at[half, way, kind], self.send2, self.recv2.at[half, min(kind, 1)],
            self.row, self.place(half, first, self.step(second, way)),
        ).start()

    def arrive(self, got, recv, half, kind):
        kinds = pl.ds(0, 1) if kind == FAR else pl.ds(1, 2)
        await_bytes(got.at[half, :, kinds], recv.at[half, kind])

    both = tuple((half, way) for half in range(2) for way in range(2))

    def open(self, fill):
        for half in range(2):
            fill(self, half, (self.spot(half)[0] + 2) % SIDE)
        for half, way in self.both:
            self.hop1(half, way, FAR)
        for way in range(2):
            for half in range(2):
                fill(self, half, self.step(self.spot(half)[0], way))
        for half, way in self.both:
            self.hop1(half, way, RAW)
        for half in range(2):
            fill(self, half, self.spot(half)[0])

    def merge1(self):
        for half, way in self.both:
            if way == 0:
                self.arrive(self.got1, self.recv1, half, FAR)
            mine = self.group(half, self.step(self.spot(half)[0], way), way)
            got = self.got1.at[half, way, FAR]

            @pl.loop(0, self.nf * SIDE)
            def _(i):
                f, j = i // SIDE, i % SIDE
                mine[f, j] = (mine[f, j].astype(jnp.float32) + got[f, j].astype(jnp.float32)).astype(BF16)

            self.hop1(half, way, MERGED)

    def turn(self):
        for half in range(2):
            second = self.spot(half)[1]
            self.arrive(self.got1, self.recv1, half, RAW)
            for h in range(2):
                mine = self.group(half, self.spot(half)[0], h)
                one, two = self.got1.at[half, h, MERGED], self.got1.at[half, 1 - h, RAW]

                @pl.loop(0, self.nf * (SIDE - 1))
                def _(i):
                    f, j = i // (SIDE - 1), (second + 1 + i % (SIDE - 1)) % SIDE
                    total = mine[f, j].astype(jnp.float32) + one[f, j].astype(jnp.float32)
                    mine[f, j] = (total + two[f, j].astype(jnp.float32)).astype(BF16)

            for way in range(2):
                self.hop2(half, way, FAR)
            for way in range(2):
                self.hop2(half, way, RAW)

    def merge2(self):
        for half, way in self.both:
            if way == 0:
                self.arrive(self.got2, self.recv2, half, FAR)
            mine = self.single(half, self.step(self.spot(half)[1], way), way)
            got = self.got2.at[half, way, FAR]
            for f in range(self.nf):
                mine[f] = (mine[f].astype(jnp.float32) + got[f].astype(jnp.float32)).astype(BF16)
            self.hop2(half, way, MERGED)

    def close(self, summed):
        for half in range(2):
            second = self.spot(half)[1]
            self.arrive(self.got2, self.recv2, half, RAW)
            for h in range(2):
                mine = self.single(half, second, h)
                for f in range(self.nf):
                    total = mine[f].astype(jnp.float32)
                    total = total + self.got1[half, h, MERGED, f, second].astype(jnp.float32)
                    total = total + self.got1[half, 1 - h, RAW, f, second].astype(jnp.float32)
                    total = total + self.got2[half, h, MERGED, f].astype(jnp.float32)
                    total = total + self.got2[half, 1 - h, RAW, f].astype(jnp.float32)
                    summed[self.f0 + f, self.lines(half, h)] = total.astype(BF16)

    def drain(self):
        await_bytes(self.got1, self.send1)
        await_bytes(self.got2, self.send2)


def kernel(x, values_hbm, tile_rows, tile_cols, tile_count, w_first, w_second, out, *scratch):
    scratch = list(scratch)

    def take(number):
        taken = scratch[:number]
        del scratch[:number]
        return taken

    values, runs, part, summed, staged, plan, plan_smem, values_sem, x_sem, plan_sem, out_sem = take(11)
    inputs, hidden = take(2), take(1)[0]
    row, col = lax.axis_index("row"), lax.axis_index("col")
    spreads = [
        [Spread(unit, panel, take(4), row, col) for unit, panel in zip(SPREADS[0], inputs)],
        [Spread(unit, hidden, take(4), row, col) for unit in SPREADS[1]],
    ]
    sums = [[Sum(unit, part, *take(2), take(4), row, col) for unit in UNITS[layer]] for layer in range(2)]

    loads = [
        pltpu.make_async_copy(
            x.at[:, :, pl.ds(f * WIDE, WIDE)], inputs[f].at[0, pl.ds(row * BLOCK_TILES, BLOCK_TILES)], x_sem.at[f]
        )
        for f in range(2)
    ]
    for load in loads:
        load.start()
    values_load = pltpu.make_async_copy(values_hbm.at[0, 0], values, values_sem)
    values_load.start()

    first_spread = spreads[0][0]
    first_sum = sums[0][0]
    partners = [(step, col) for step in first_spread.steps] + [(first_spread.mate, col)]
    for half, way in Sum.both:
        first, second = first_sum.spot(half)
        partners.append((row, first_sum.place(half, first_sum.step(first, way), second)))
    barrier = pltpu.get_barrier_semaphore()
    for to_row, to_col in partners:
        pl.semaphore_signal(barrier, inc=1, device_id=(to_row, to_col), device_id_type=MESH)
    pl.semaphore_wait(barrier, len(partners))
    loads[0].wait()
    spreads[0][0].own()

    lane = lax.broadcasted_iota(jnp.int32, (1, SLOTS), 1)
    key = jnp.where(lane < tile_count[0, 0], tile_rows[0] * 64 + tile_cols[0], lane + 8192)
    across = jnp.broadcast_to(key.astype(jnp.float32), (SLOTS, SLOTS))
    down = jnp.transpose(across)
    rank = jnp.sum(jnp.where(across < down, 1.0, 0.0), axis=1, keepdims=True)
    lanes = lax.broadcasted_iota(jnp.int32, (SLOTS, SLOTS), 1)
    slots = lax.broadcasted_iota(jnp.int32, (SLOTS, SLOTS), 0).astype(jnp.float32)
    chosen = rank == lanes.astype(jnp.float32)
    order = jnp.sum(jnp.where(chosen, slots, 0.0), axis=0, keepdims=True)
    ordered = jnp.sum(jnp.where(chosen, down, 0.0), axis=0, keepdims=True)
    ends = jnp.sum(jnp.where(down < ((lanes + 1) * 64).astype(jnp.float32), 1.0, 0.0), axis=0, keepdims=True)
    rest = jnp.zeros((5, SLOTS), jnp.float32)
    plan[...] = jnp.concatenate([order, ordered, ends, rest], axis=0).astype(jnp.int32)
    for f in range(2):
        runs[f, SLOTS] = jnp.zeros((TILE, WIDE), BF16)
    plan_copy = pltpu.make_async_copy(plan, plan_smem, plan_sem)
    plan_copy.start()

    def multiply(panel, f, f0, first, last, total):
        def block(it, total):
            for u in range(UNROLL):
                at = it * UNROLL + u
                slot = jnp.clip(plan_smem[0, at], 0, SLOTS - 1)
                key = jnp.clip(plan_smem[1, at], 0, 64 * SLOTS - 1)
                before = plan_smem[1, jnp.maximum(at - 1, 0)]
                keep = jnp.where(key // 64 == before // 64, 1.0, 0.0)
                right = panel[f, key % 64]
                total = total * keep + jnp.dot(values[slot], right, preferred_element_type=jnp.float32)
                runs[f0, at] = total.astype(BF16)
            return total

        return lax.fori_loop(first // UNROLL, last // UNROLL, block, total)

    empty = jnp.zeros((TILE, WIDE), jnp.float32)

    def fill(unit, half, first):
        tiles = unit.rows // 2 // TILE
        base = unit.r0 // TILE + half * tiles

        @pl.loop(0, SIDE * tiles)
        def _(i):
            second, t = i // tiles, base + i % tiles
            up, across = (second, first) if half == 0 else (first, second)
            line = (up * SIDE + across) * BLOCK_TILES + t
            end = plan_smem[2, line]
            start = jnp.where(line == 0, 0, plan_smem[2, jnp.maximum(line - 1, 0)])
            run = jnp.clip(jnp.where(end == start, SLOTS, end - 1), 0, SLOTS)
            for f in range(unit.nf):
                part[unit.f0 + f, up, across, pl.ds(pl.multiple_of(t * TILE, TILE), TILE)] = runs[unit.f0 + f, run]

    def weigh(unit, w, store):
        @pl.loop(0, unit.rows // TILE)
        def _(i):
            t = unit.r0 // TILE + i
            lines = pl.ds(pl.multiple_of(t * TILE, TILE), TILE)
            both = jnp.concatenate([summed[0, lines], summed[1, lines]], axis=1)
            product = jnp.dot(both, w[...], preferred_element_type=jnp.float32)
            store(t, jnp.maximum(product, 0.0).astype(BF16))

    def keep_hidden(t, block):
        for f in range(2):
            hidden[f, row * BLOCK_TILES + t] = block[:, f * WIDE : (f + 1) * WIDE]

    def keep_output(t, block):
        staged[pl.ds(pl.multiple_of(t * TILE, TILE), TILE)] = block

    def write(unit):
        lines = pl.ds(unit.r0, unit.rows)
        return pltpu.make_async_copy(staged.at[lines], out.at[lines], out_sem.at[unit.r0 // 512])

    a, b = spreads[0]
    a0, a1, b0, b1, b2, b3 = sums[0]
    g0, g1, g2, g3 = spreads[1]
    a.onward(0)
    loads[1].wait()
    b.own()
    a.onward(1)
    a.onward(2)
    plan_copy.wait()
    values_load.wait()
    a.finish()
    total = multiply(inputs[0], 0, 0, 0, 128, empty)
    b.onward(0)
    total = multiply(inputs[0], 0, 0, 128, 256, total)
    a1.open(fill)
    b.onward(1)
    a0.open(fill)
    b.onward(2)
    b.finish()
    total = multiply(inputs[1], 0, 1, 0, 256, empty)
    a0.merge1()
    b0.open(fill)
    b1.open(fill)
    a0.turn()
    b1.merge1()
    b0.merge1()
    a0.merge2()
    a1.merge1()
    b0.turn()
    b1.turn()
    b2.open(fill)
    b0.merge2()
    a0.close(summed)
    b1.merge2()
    b3.open(fill)
    b2.merge1()
    b1.close(summed)
    weigh(b1, w_first, keep_hidden)
    b0.close(summed)
    g1.own()
    weigh(b0, w_first, keep_hidden)
    g0.own()
    b3.merge1()
    a1.turn()
    b2.turn()
    b3.turn()
    a1.merge2()
    b2.merge2()
    g1.onward(0)
    g0.onward(0)
    b3.merge2()
    a1.close(summed)
    b2.close(summed)
    weigh(b2, w_first, keep_hidden)
    g2.own()
    g0.onward(1)
    g1.onward(1)
    b3.close(summed)
    weigh(b3, w_first, keep_hidden)
    g3.own()
    g0.onward(2)
    g1.onward(2)
    g0.finish()
    g1.finish()
    g2.onward(0)
    g2.onward(1)
    g3.onward(0)
    g3.onward(1)
    g2.onward(2)
    g2.finish()
    g3.onward(2)
    for unit in sums[0]:
        unit.drain()
    g3.finish()

    d, e0, e1 = sums[1]
    total = multiply(hidden, 0, 0, 0, 256, empty)
    d.open(fill)
    total = multiply(hidden, 1, 1, 0, 128, empty)
    d.merge1()
    total = multiply(hidden, 1, 1, 128, 256, total)
    e1.open(fill)
    e0.open(fill)
    e1.merge1()
    e0.merge1()
    d.turn()
    e1.turn()
    e0.turn()
    d.merge2()
    e1.merge2()
    e0.merge2()
    d.close(summed)
    e1.close(summed)
    weigh(e1, w_second, keep_output)
    write(e1).start()
    e0.close(summed)
    weigh(e0, w_second, keep_output)
    write(e0).start()
    for unit in spreads[0] + spreads[1] + sums[1]:
        unit.drain()
    write(e0).wait()
    write(e1).wait()


def both_layers(x, values, rows, cols, count, w_first, w_second):
    vmem, smem = pl.BlockSpec(memory_space=pltpu.VMEM), pl.BlockSpec(memory_space=pltpu.SMEM)
    hbm = pl.BlockSpec(memory_space=pl.ANY)
    dma = pltpu.SemaphoreType.DMA
    scratch = [
        pltpu.VMEM((SLOTS, TILE, TILE), BF16),
        pltpu.VMEM((2, SLOTS + 1, TILE, WIDE), BF16),
        pltpu.VMEM((2, SIDE, SIDE, NODES, WIDE), BF16),
        pltpu.VMEM((2, NODES, WIDE), BF16),
        pltpu.VMEM((NODES, F), BF16),
        pltpu.VMEM((8, SLOTS), jnp.int32),
        pltpu.SMEM((8, SLOTS), jnp.int32),
        dma,
        dma((2,)),
        dma,
        dma((2,)),
    ]
    scratch += [pltpu.VMEM((halves, 64, TILE, WIDE), BF16) for halves in (1, 1, 2)]
    for layer in range(2):
        for _ in SPREADS[layer]:
            scratch += [dma, dma((3,)), dma, dma]
    for layer in range(2):
        for _, nf, _, rows_of in UNITS[layer]:
            scratch += [
                pltpu.VMEM((2, 2, 3, nf, SIDE, rows_of // 4, WIDE), BF16),
                pltpu.VMEM((2, 2, 3, nf, rows_of // 4, WIDE), BF16),
                dma, dma((2, 2)), dma, dma((2, 2)),
            ]
    return pl.pallas_call(
        kernel,
        out_shape=jax.ShapeDtypeStruct((NODES, F), BF16),
        in_specs=[hbm, hbm, vmem, vmem, smem, vmem, vmem],
        out_specs=hbm,
        scratch_shapes=scratch,
        compiler_params=pltpu.CompilerParams(
            collective_id=0, has_side_effects=True, vmem_limit_bytes=67043328
        ),
        name="layers",
    )(x, values, rows, cols, count, w_first, w_second)


def shards(features, tile_values, tile_rows, tile_cols, tile_count, w_first, w_second):
    return both_layers(
        features.reshape(BLOCK_TILES, TILE, F), tile_values, tile_rows[0], tile_cols[0], tile_count, w_first, w_second
    )


def solution(mesh):
    return jax.shard_map(
        shards,
        mesh=mesh,
        in_specs=(
            P(("row", "col"), None),
            P("row", "col", None, None, None),
            P("row", "col", None),
            P("row", "col", None),
            P("row", "col"),
            P(),
            P(),
        ),
        out_specs=P(("row", "col"), None),
        check_vma=False,
    )
```

```python
import jax
import jax.numpy as jnp
from jax import lax
from jax.experimental import pallas as pl
from jax.experimental.pallas import tpu as pltpu
from jax.sharding import PartitionSpec as P

MESH = pl.DeviceIdType.MESH
F = 256
WIDE = 128
TILE = 128
SLOTS = 256
NODES = 1024
SIDE = 4
BLOCK_TILES = NODES // TILE
UNROLL = 32
FAR, RAW, MERGED = 0, 1, 2
BF16 = jnp.bfloat16

UNITS = (
    ((0, 1, 0, 512), (0, 1, 512, 512), (1, 1, 0, 256), (1, 1, 256, 256), (1, 1, 512, 256), (1, 1, 768, 256)),
    ((0, 1, 0, 1024), (1, 1, 0, 512), (1, 1, 512, 512)),
)
SPREADS = (((0, 8),), ((0, 2), (2, 2), (4, 2), (6, 2)))


def remote(src, dst, send, recv, row, col):
    return pltpu.make_async_remote_copy(
        src_ref=src, dst_ref=dst, send_sem=send, recv_sem=recv, device_id=(row, col), device_id_type=MESH
    )


def await_bytes(sized, sem):
    pltpu.make_async_copy(sized, sized, sem).wait()


class Spread:
    def __init__(self, unit, panel, sems, row, col):
        self.t0, self.tiles = unit
        self.panel, self.row, self.col = panel, row, col
        self.recv, self.send, self.mate_recv = sems
        self.z, self.core = row // 2, row % 2
        self.mate = self.z * 2 + 1 - self.core
        self.steps = ((self.z + 1) % SIDE * 2 + self.core, (self.z + 3) % SIDE * 2 + self.core)
        self.groups = (((3, 0), (1, 1)), ((3, 1), (1, 0)), ((2, 0), (2, 1)))

    def at(self, distance, core):
        return (self.z + distance) % SIDE * 2 + core

    def part(self, block, which):
        half = self.tiles // 2
        return self.panel.at[pl.ds(block * BLOCK_TILES + self.t0 + which * half, half)]

    def sized(self, tiles):
        return self.panel.at[pl.ds(0, tiles)]

    def hop(self, way, order, block, which):
        piece = self.part(block, which)
        remote(piece, piece, self.send, self.recv.at[order], self.steps[way], self.col).start()

    def share(self, block, which):
        piece = self.part(block, which)
        remote(piece, piece, self.send, self.mate_recv, self.mate, self.col).start()

    def own(self):
        for order in range(2):
            for way in range(2):
                self.hop(way, order, self.row, way ^ order)
        for which in range(2):
            self.share(self.row, which)

    def onward(self, order):
        await_bytes(self.sized(self.tiles), self.recv.at[order])
        for way in range(2):
            distance, which = self.groups[order][way]
            block = self.at(distance, self.core)
            if order == 0:
                self.hop(way, 2, block, which)
            self.share(block, which)


class Sum:
    def __init__(self, unit, part, got1, got2, sems, row, col):
        self.f0, self.nf, self.r0, self.rows = unit
        self.quarter = self.rows // 4
        self.part, self.got1, self.got2 = part, got1, got2
        self.recv1, self.recv2, self.send = sems
        self.row = row
        self.y, self.x = col // SIDE, col % SIDE

    def spot(self, half):
        return (self.x, self.y) if half == 0 else (self.y, self.x)

    def step(self, at, way):
        return (at + (1 if way == 0 else SIDE - 1)) % SIDE

    def place(self, half, first, second):
        return second * SIDE + first if half == 0 else first * SIDE + second

    def lines(self, half, h):
        return pl.ds(self.r0 + (2 * half + h) * self.quarter, self.quarter)

    def group(self, half, first, h):
        halves = pl.ds(self.f0, self.nf)
        if half == 0:
            return self.part.at[halves, :, first, self.lines(half, h)]
        return self.part.at[halves, first, :, self.lines(half, h)]

    def single(self, half, second, h):
        halves = pl.ds(self.f0, self.nf)
        first = self.spot(half)[0]
        if half == 0:
            return self.part.at[halves, second, first, self.lines(half, h)]
        return self.part.at[halves, first, second, self.lines(half, h)]

    def hop1(self, half, way, kind):
        first, second = self.spot(half)
        if kind == FAR:
            src = self.group(half, (first + 2) % SIDE, way)
        elif kind == RAW:
            src = self.group(half, self.step(first, way), 1 - way)
        else:
            src = self.group(half, self.step(first, way), way)
        remote(
            src, self.got1.at[half, way, kind], self.send, self.recv1.at[half, min(kind, 1)],
            self.row, self.place(half, self.step(first, way), second),
        ).start()

    def hop2(self, half, way, kind):
        first, second = self.spot(half)
        if kind == FAR:
            src = self.single(half, (second + 2) % SIDE, way)
        elif kind == RAW:
            src = self.single(half, self.step(second, way), 1 - way)
        else:
            src = self.single(half, self.step(second, way), way)
        remote(
            src, self.got2.at[half, way, kind], self.send, self.recv2.at[half, min(kind, 1)],
            self.row, self.place(half, first, self.step(second, way)),
        ).start()

    def arrive(self, got, recv, half, kind):
        kinds = pl.ds(0, 1) if kind == FAR else pl.ds(1, 2)
        await_bytes(got.at[half, :, kinds], recv.at[half, kind])

    both = tuple((half, way) for half in range(2) for way in range(2))

    def open(self, fill):
        for half in range(2):
            fill(self, half, (self.spot(half)[0] + 2) % SIDE)
        for half, way in self.both:
            self.hop1(half, way, FAR)
        for way in range(2):
            for half in range(2):
                fill(self, half, self.step(self.spot(half)[0], way))
        for half, way in self.both:
            self.hop1(half, way, RAW)
        for half in range(2):
            fill(self, half, self.spot(half)[0])

    def merge1(self):
        for half, way in self.both:
            if way == 0:
                self.arrive(self.got1, self.recv1, half, FAR)
            mine = self.group(half, self.step(self.spot(half)[0], way), way)
            got = self.got1.at[half, way, FAR]

            @pl.loop(0, self.nf * SIDE)
            def _(i):
                f, j = i // SIDE, i % SIDE
                mine[f, j] = (mine[f, j].astype(jnp.float32) + got[f, j].astype(jnp.float32)).astype(BF16)

            self.hop1(half, way, MERGED)

    def turn(self):
        for half in range(2):
            second = self.spot(half)[1]
            self.arrive(self.got1, self.recv1, half, RAW)
            for h in range(2):
                mine = self.group(half, self.spot(half)[0], h)
                one, two = self.got1.at[half, h, MERGED], self.got1.at[half, 1 - h, RAW]

                @pl.loop(0, self.nf * (SIDE - 1))
                def _(i):
                    f, j = i // (SIDE - 1), (second + 1 + i % (SIDE - 1)) % SIDE
                    total = mine[f, j].astype(jnp.float32) + one[f, j].astype(jnp.float32)
                    mine[f, j] = (total + two[f, j].astype(jnp.float32)).astype(BF16)

            for way in range(2):
                self.hop2(half, way, FAR)
            for way in range(2):
                self.hop2(half, way, RAW)

    def merge2(self):
        for half, way in self.both:
            if way == 0:
                self.arrive(self.got2, self.recv2, half, FAR)
            mine = self.single(half, self.step(self.spot(half)[1], way), way)
            got = self.got2.at[half, way, FAR]
            for f in range(self.nf):
                mine[f] = (mine[f].astype(jnp.float32) + got[f].astype(jnp.float32)).astype(BF16)
            self.hop2(half, way, MERGED)

    def close(self, summed):
        for half in range(2):
            second = self.spot(half)[1]
            self.arrive(self.got2, self.recv2, half, RAW)
            for h in range(2):
                mine = self.single(half, second, h)
                for f in range(self.nf):
                    total = mine[f].astype(jnp.float32)
                    total = total + self.got1[half, h, MERGED, f, second].astype(jnp.float32)
                    total = total + self.got1[half, 1 - h, RAW, f, second].astype(jnp.float32)
                    total = total + self.got2[half, h, MERGED, f].astype(jnp.float32)
                    total = total + self.got2[half, 1 - h, RAW, f].astype(jnp.float32)
                    summed[self.f0 + f, self.lines(half, h)] = total.astype(BF16)


def kernel(x, values_hbm, rows_hbm, cols_hbm, tile_count, w_first_hbm, w_second_hbm, out, *scratch):
    scratch = list(scratch)

    def take(number):
        taken = scratch[:number]
        del scratch[:number]
        return taken

    values, runs, part, summed, staged, plan, plan_smem, tile_rows, tile_cols, w_first, w_second = take(11)
    values_sem, x_sem, plan_sem, out_sem, small_sem, spread_send, share_recv, sum_send = take(8)
    panels = [take(2), take(2)]
    row, col = lax.axis_index("row"), lax.axis_index("col")
    spreads = [
        [
            [
                Spread(unit, panels[layer][f], take(1) + [spread_send, share_recv.at[layer, f]], row, col)
                for unit in SPREADS[layer]
            ]
            for f in range(2)
        ]
        for layer in range(2)
    ]
    sums = [
        [Sum(unit, part, *take(2), take(2) + [sum_send.at[layer]], row, col) for unit in UNITS[layer]]
        for layer in range(2)
    ]

    first_spread = spreads[0][0][0]
    first_sum = sums[0][0]
    partners = [(step, col) for step in first_spread.steps] + [(first_spread.mate, col)]
    for half, way in Sum.both:
        first, second = first_sum.spot(half)
        partners.append((row, first_sum.place(half, first_sum.step(first, way), second)))
    barrier = pltpu.get_barrier_semaphore()
    for to_row, to_col in partners:
        pl.semaphore_signal(barrier, inc=1, device_id=(to_row, to_col), device_id_type=MESH)

    loads = [
        pltpu.make_async_copy(
            x.at[:, :, pl.ds(f * WIDE, WIDE)], panels[0][f].at[pl.ds(row * BLOCK_TILES, BLOCK_TILES)], x_sem.at[f]
        )
        for f in range(2)
    ]
    small = [
        pltpu.make_async_copy(source, target, small_sem.at[i])
        for i, (source, target) in enumerate(
            ((rows_hbm, tile_rows), (cols_hbm, tile_cols), (w_first_hbm, w_first), (w_second_hbm, w_second))
        )
    ]
    for copy in [loads[0]] + small[:2] + [loads[1]] + small[2:]:
        copy.start()
    values_load = pltpu.make_async_copy(values_hbm.at[0, 0], values, values_sem)
    values_load.start()
    pl.semaphore_wait(barrier, len(partners))
    loads[0].wait()
    spreads[0][0][0].own()
    for copy in small:
        copy.wait()

    lane = lax.broadcasted_iota(jnp.int32, (1, SLOTS), 1)
    key = jnp.where(lane < tile_count[0, 0], tile_rows[...] * 64 + tile_cols[...], lane + 8192)
    across = jnp.broadcast_to(key.astype(jnp.float32), (SLOTS, SLOTS))
    down = jnp.transpose(across)
    rank = jnp.sum(jnp.where(across < down, 1.0, 0.0), axis=1, keepdims=True)
    lanes = lax.broadcasted_iota(jnp.int32, (SLOTS, SLOTS), 1).astype(jnp.float32)
    slots = lax.broadcasted_iota(jnp.int32, (SLOTS, SLOTS), 0).astype(jnp.float32)

    def pick(condition, what):
        return jnp.sum(jnp.where(condition, what, 0.0), axis=0, keepdims=True).astype(jnp.int32)

    order = pick(rank == lanes, slots)
    ordered = pick(rank == lanes, down)
    before = pick(rank == lanes - 1.0, down)
    ends = pick(down < (lanes + 1.0) * 64.0, 1.0)
    starts = pick(down < lanes * 64.0, 1.0)
    same = jnp.where(jnp.right_shift(ordered, 6) == jnp.right_shift(before, 6), 1, 0)
    run_of = jnp.where(ends == starts, SLOTS, ends - 1)
    rest = jnp.zeros((4, SLOTS), jnp.int32)
    plan[...] = jnp.concatenate([order, jnp.bitwise_and(ordered, 63), run_of, same, rest], axis=0)
    for f in range(2):
        runs[f, SLOTS] = jnp.zeros((TILE, WIDE), BF16)
    plan_copy = pltpu.make_async_copy(plan, plan_smem, plan_sem)
    plan_copy.start()

    def multiply(panel, f, first, last, total):
        def block(it, total):
            for u in range(UNROLL):
                at = it * UNROLL + u
                slot = jnp.clip(plan_smem[0, at], 0, SLOTS - 1)
                column = jnp.clip(plan_smem[1, at], 0, 63)
                keep = jnp.where(plan_smem[3, at] == 1, 1.0, 0.0)
                total = total * keep + jnp.dot(values[slot], panel[column], preferred_element_type=jnp.float32)
                runs[f, at] = total.astype(BF16)
            return total

        return lax.fori_loop(first // UNROLL, last // UNROLL, block, total)

    empty = jnp.zeros((TILE, WIDE), jnp.float32)

    def fill(unit, half, first):
        tiles = unit.rows // 2 // TILE
        base = unit.r0 // TILE + half * tiles

        @pl.loop(0, SIDE, unroll=SIDE if tiles == 1 else 1)
        def _(second):
            up, across = (second, first) if half == 0 else (first, second)
            for t in range(base, base + tiles):
                run = jnp.clip(plan_smem[2, (up * SIDE + across) * BLOCK_TILES + t], 0, SLOTS)
                for f in range(unit.f0, unit.f0 + unit.nf):
                    part[f, up, across, pl.ds(t * TILE, TILE)] = runs[f, run]

    def weigh(unit, w, store):
        @pl.loop(0, unit.rows // TILE, unroll=unit.rows // TILE)
        def _(i):
            t = unit.r0 // TILE + i
            lines = pl.ds(pl.multiple_of(t * TILE, TILE), TILE)
            both = jnp.concatenate([summed[0, lines], summed[1, lines]], axis=1)
            product = jnp.dot(both, w[...], preferred_element_type=jnp.float32)
            store(t, jnp.maximum(product, 0.0).astype(BF16))

    def keep_hidden(t, block):
        for f in range(2):
            panels[1][f][row * BLOCK_TILES + t] = block[:, f * WIDE : (f + 1) * WIDE]

    def write(t):
        lines = pl.ds(pl.multiple_of(t * TILE, TILE), TILE)
        return pltpu.make_async_copy(staged.at[lines], out.at[lines], out_sem)

    def keep_output(t, block):
        staged[pl.ds(pl.multiple_of(t * TILE, TILE), TILE)] = block
        write(t).start()

    def shared(layer, f):
        await_bytes(panels[layer][f].at[pl.ds(0, 32)], share_recv.at[layer, f])

    (a,), (b,) = spreads[0]
    a0, a1, b0, b1, b2, b3 = sums[0]
    (g0, g1, g2, g3), (h0, h1, h2, h3) = spreads[1]
    d, e0, e1 = sums[1]
    a.onward(0)
    loads[1].wait()
    b.own()
    a.onward(1)
    a.onward(2)
    shared(0, 0)
    plan_copy.wait()
    values_load.wait()
    total = multiply(panels[0][0], 0, 0, 128, empty)
    total = multiply(panels[0][0], 0, 128, 256, total)
    a0.open(fill)
    b.onward(0)
    b.onward(1)
    a0.merge1()
    b.onward(2)
    shared(0, 1)
    a1.open(fill)
    total = multiply(panels[0][1], 1, 0, 128, empty)
    total = multiply(panels[0][1], 1, 128, 256, total)
    b1.open(fill)
    a0.turn()
    b0.open(fill)
    b1.merge1()
    b0.merge1()
    b2.open(fill)
    b0.turn()
    a0.merge2()
    a1.merge1()
    b0.merge2()
    b1.turn()
    a0.close(summed)
    b3.open(fill)
    b0.close(summed)
    b1.merge2()
    weigh(b0, w_first, keep_hidden)
    h0.own()
    b2.merge1()
    b3.merge1()
    a1.turn()
    g0.own()
    b1.close(summed)
    weigh(b1, w_first, keep_hidden)
    g1.own()
    b2.turn()
    h1.own()
    b3.turn()
    a1.merge2()
    g0.onward(0)
    b2.merge2()
    b3.merge2()
    h1.onward(0)
    h1.onward(1)
    g1.onward(0)
    a1.close(summed)
    b2.close(summed)
    weigh(b2, w_first, keep_hidden)
    g0.onward(1)
    g1.onward(1)
    g2.own()
    b3.close(summed)
    weigh(b3, w_first, keep_hidden)
    g3.own()
    h2.own()
    g2.onward(0)
    g3.onward(0)
    h3.own()
    h0.onward(0)
    g1.onward(2)
    g2.onward(1)
    g0.onward(2)
    g3.onward(1)
    g2.onward(2)
    h1.onward(2)
    h0.onward(1)
    h2.onward(0)
    g3.onward(2)
    h3.onward(0)
    h2.onward(1)
    shared(1, 0)
    await_bytes(values.at[pl.ds(0, 240)], sum_send.at[0])

    total = multiply(panels[1][0], 0, 0, 128, empty)
    h2.onward(2)
    h0.onward(2)
    h3.onward(1)
    total = multiply(panels[1][0], 0, 128, 256, total)
    h3.onward(2)
    d.open(fill)
    shared(1, 1)
    total = multiply(panels[1][1], 1, 0, 128, empty)
    d.merge1()
    total = multiply(panels[1][1], 1, 128, 256, total)
    e1.open(fill)
    e0.open(fill)
    e1.merge1()
    e0.merge1()
    d.turn()
    e1.turn()
    e0.turn()
    d.merge2()
    e1.merge2()
    e0.merge2()
    d.close(summed)
    e1.close(summed)
    weigh(e1, w_second, keep_output)
    e0.close(summed)
    weigh(e0, w_second, keep_output)
    await_bytes(values.at[pl.ds(0, 224)], spread_send)
    await_bytes(values.at[pl.ds(0, 240)], sum_send.at[1])
    await_bytes(staged, out_sem)


def both_layers(x, values, rows, cols, count, w_first, w_second):
    smem, hbm = pl.BlockSpec(memory_space=pltpu.SMEM), pl.BlockSpec(memory_space=pl.ANY)
    dma = pltpu.SemaphoreType.DMA
    scratch = [
        pltpu.VMEM((SLOTS, TILE, TILE), BF16),
        pltpu.VMEM((2, SLOTS + 1, TILE, WIDE), BF16),
        pltpu.VMEM((2, SIDE, SIDE, NODES, WIDE), BF16),
        pltpu.VMEM((2, NODES, WIDE), BF16),
        pltpu.VMEM((NODES, F), BF16),
        pltpu.VMEM((8, SLOTS), jnp.int32),
        pltpu.SMEM((8, SLOTS), jnp.int32),
        pltpu.VMEM((1, SLOTS), jnp.int32),
        pltpu.VMEM((1, SLOTS), jnp.int32),
        pltpu.VMEM((F, F), BF16),
        pltpu.VMEM((F, F), BF16),
        dma,
        dma((2,)),
        dma,
        dma,
        dma((4,)),
        dma,
        dma((2, 2)),
        dma((2,)),
    ]
    scratch += [pltpu.VMEM((64, TILE, WIDE), BF16)] * 4
    for layer in range(2):
        for _ in SPREADS[layer] * 2:
            scratch += [dma((3,))]
    for layer in range(2):
        for _, nf, _, rows_of in UNITS[layer]:
            scratch += [
                pltpu.VMEM((2, 2, 3, nf, SIDE, rows_of // 4, WIDE), BF16),
                pltpu.VMEM((2, 2, 3, nf, rows_of // 4, WIDE), BF16),
                dma((2, 2)), dma((2, 2)),
            ]
    return pl.pallas_call(
        kernel,
        out_shape=jax.ShapeDtypeStruct((NODES, F), BF16),
        in_specs=[hbm, hbm, hbm, hbm, smem, hbm, hbm],
        out_specs=hbm,
        scratch_shapes=scratch,
        compiler_params=pltpu.CompilerParams(
            collective_id=0, has_side_effects=True, vmem_limit_bytes=67043328
        ),
        name="layers",
    )(x, values, rows, cols, count, w_first, w_second)


def shards(features, tile_values, tile_rows, tile_cols, tile_count, w_first, w_second):
    return both_layers(
        features.reshape(BLOCK_TILES, TILE, F), tile_values, tile_rows[0], tile_cols[0], tile_count, w_first, w_second
    )


def solution(mesh):
    return jax.shard_map(
        shards,
        mesh=mesh,
        in_specs=(
            P(("row", "col"), None),
            P("row", "col", None, None, None),
            P("row", "col", None),
            P("row", "col", None),
            P("row", "col"),
            P(),
            P(),
        ),
        out_specs=P(("row", "col"), None),
        check_vma=False,
    )
```

```python
import jax
import jax.numpy as jnp
from jax import lax
from jax.experimental import pallas as pl
from jax.experimental.pallas import tpu as pltpu
from jax.sharding import PartitionSpec as P

MESH = pl.DeviceIdType.MESH
F = 256
WIDE = 128
TILE = 128
SLOTS = 256
NODES = 1024
SIDE = 4
BLOCK_TILES = NODES // TILE
UNROLL = 128
FAR, RAW, MERGED = 0, 1, 2
BF16 = jnp.bfloat16

UNITS = (
    ((0, 1, 0, 512), (0, 1, 512, 512), (1, 1, 0, 256), (1, 1, 256, 256), (1, 1, 512, 256), (1, 1, 768, 256)),
    ((0, 1, 0, 1024), (1, 1, 0, 512), (1, 1, 512, 512)),
)
SPREADS = (((0, 8),), ((0, 2), (2, 2), (4, 2), (6, 2)))


def remote(src, dst, send, recv, row, col):
    return pltpu.make_async_remote_copy(
        src_ref=src, dst_ref=dst, send_sem=send, recv_sem=recv, device_id=(row, col), device_id_type=MESH
    )


def await_bytes(sized, sem):
    pltpu.make_async_copy(sized, sized, sem).wait()


class Spread:
    def __init__(self, unit, panel, sems, row, col):
        self.t0, self.tiles = unit
        self.panel, self.row, self.col = panel, row, col
        self.recv, self.send, self.mate_recv = sems
        self.z, self.core = row // 2, row % 2
        self.mate = self.z * 2 + 1 - self.core
        self.steps = ((self.z + 1) % SIDE * 2 + self.core, (self.z + 3) % SIDE * 2 + self.core)
        self.groups = (((3, 0), (1, 1)), ((3, 1), (1, 0)), ((2, 0), (2, 1)))

    def at(self, distance, core):
        return (self.z + distance) % SIDE * 2 + core

    def part(self, block, which):
        half = self.tiles // 2
        return self.panel.at[pl.ds(block * BLOCK_TILES + self.t0 + which * half, half)]

    def sized(self, tiles):
        return self.panel.at[pl.ds(0, tiles)]

    def hop(self, way, order, block, which):
        piece = self.part(block, which)
        remote(piece, piece, self.send, self.recv.at[order], self.steps[way], self.col).start()

    def share(self, block, which):
        piece = self.part(block, which)
        remote(piece, piece, self.send, self.mate_recv, self.mate, self.col).start()

    def own(self):
        for order in range(2):
            for way in range(2):
                self.hop(way, order, self.row, way ^ order)
        for which in range(2):
            self.share(self.row, which)

    def onward(self, order):
        await_bytes(self.sized(self.tiles), self.recv.at[order])
        for way in range(2):
            distance, which = self.groups[order][way]
            block = self.at(distance, self.core)
            if order == 0:
                self.hop(way, 2, block, which)
            self.share(block, which)


class Sum:
    def __init__(self, unit, part, got1, got2, sems, row, col):
        self.f0, self.nf, self.r0, self.rows = unit
        self.quarter = self.rows // 4
        self.part, self.got1, self.got2 = part, got1, got2
        self.recv1, self.recv2, self.send = sems
        self.row = row
        self.y, self.x = col // SIDE, col % SIDE

    def spot(self, half):
        return (self.x, self.y) if half == 0 else (self.y, self.x)

    def step(self, at, way):
        return (at + (1 if way == 0 else SIDE - 1)) % SIDE

    def place(self, half, first, second):
        return second * SIDE + first if half == 0 else first * SIDE + second

    def lines(self, half, h):
        return pl.ds(self.r0 + (2 * half + h) * self.quarter, self.quarter)

    def group(self, half, first, h):
        halves = pl.ds(self.f0, self.nf)
        if half == 0:
            return self.part.at[halves, :, first, self.lines(half, h)]
        return self.part.at[halves, first, :, self.lines(half, h)]

    def single(self, half, second, h):
        halves = pl.ds(self.f0, self.nf)
        first = self.spot(half)[0]
        if half == 0:
            return self.part.at[halves, second, first, self.lines(half, h)]
        return self.part.at[halves, first, second, self.lines(half, h)]

    def hop1(self, half, way, kind):
        first, second = self.spot(half)
        if kind == FAR:
            src = self.group(half, (first + 2) % SIDE, way)
        elif kind == RAW:
            src = self.group(half, self.step(first, way), 1 - way)
        else:
            src = self.group(half, self.step(first, way), way)
        remote(
            src, self.got1.at[half, way, kind], self.send, self.recv1.at[half, min(kind, 1)],
            self.row, self.place(half, self.step(first, way), second),
        ).start()

    def hop2(self, half, way, kind):
        first, second = self.spot(half)
        if kind == FAR:
            src = self.single(half, (second + 2) % SIDE, way)
        elif kind == RAW:
            src = self.single(half, self.step(second, way), 1 - way)
        else:
            src = self.single(half, self.step(second, way), way)
        remote(
            src, self.got2.at[half, way, kind], self.send, self.recv2.at[half, min(kind, 1)],
            self.row, self.place(half, first, self.step(second, way)),
        ).start()

    def arrive(self, got, recv, half, kind):
        kinds = pl.ds(0, 1) if kind == FAR else pl.ds(1, 2)
        await_bytes(got.at[half, :, kinds], recv.at[half, kind])

    both = tuple((half, way) for half in range(2) for way in range(2))

    def open(self, fill):
        for half in range(2):
            fill(self, half, (self.spot(half)[0] + 2) % SIDE)
        for half, way in self.both:
            self.hop1(half, way, FAR)
        for way in range(2):
            for half in range(2):
                fill(self, half, self.step(self.spot(half)[0], way))
        for half, way in self.both:
            self.hop1(half, way, RAW)
        for half in range(2):
            fill(self, half, self.spot(half)[0])

    def merge1(self):
        for half, way in self.both:
            if way == 0:
                self.arrive(self.got1, self.recv1, half, FAR)
            mine = self.group(half, self.step(self.spot(half)[0], way), way)
            got = self.got1.at[half, way, FAR]

            @pl.loop(0, self.nf * SIDE)
            def _(i):
                f, j = i // SIDE, i % SIDE
                mine[f, j] = (mine[f, j].astype(jnp.float32) + got[f, j].astype(jnp.float32)).astype(BF16)

            self.hop1(half, way, MERGED)

    def turn(self):
        for half in range(2):
            second = self.spot(half)[1]
            self.arrive(self.got1, self.recv1, half, RAW)
            for h in range(2):
                mine = self.group(half, self.spot(half)[0], h)
                one, two = self.got1.at[half, h, MERGED], self.got1.at[half, 1 - h, RAW]

                @pl.loop(0, self.nf * (SIDE - 1))
                def _(i):
                    f, j = i // (SIDE - 1), (second + 1 + i % (SIDE - 1)) % SIDE
                    total = mine[f, j].astype(jnp.float32) + one[f, j].astype(jnp.float32)
                    mine[f, j] = (total + two[f, j].astype(jnp.float32)).astype(BF16)

            for way in range(2):
                self.hop2(half, way, FAR)
            for way in range(2):
                self.hop2(half, way, RAW)

    def merge2(self):
        for half, way in self.both:
            if way == 0:
                self.arrive(self.got2, self.recv2, half, FAR)
            mine = self.single(half, self.step(self.spot(half)[1], way), way)
            got = self.got2.at[half, way, FAR]
            for f in range(self.nf):
                mine[f] = (mine[f].astype(jnp.float32) + got[f].astype(jnp.float32)).astype(BF16)
            self.hop2(half, way, MERGED)

    def close(self, summed):
        for half in range(2):
            second = self.spot(half)[1]
            self.arrive(self.got2, self.recv2, half, RAW)
            for h in range(2):
                mine = self.single(half, second, h)
                for f in range(self.nf):
                    total = mine[f].astype(jnp.float32)
                    total = total + self.got1[half, h, MERGED, f, second].astype(jnp.float32)
                    total = total + self.got1[half, 1 - h, RAW, f, second].astype(jnp.float32)
                    total = total + self.got2[half, h, MERGED, f].astype(jnp.float32)
                    total = total + self.got2[half, 1 - h, RAW, f].astype(jnp.float32)
                    summed[self.f0 + f, self.lines(half, h)] = total.astype(BF16)


def kernel(x, values_hbm, rows_hbm, cols_hbm, tile_count, w_first_hbm, w_second_hbm, out, *scratch):
    scratch = list(scratch)

    def take(number):
        taken = scratch[:number]
        del scratch[:number]
        return taken

    values, runs, part, summed, staged, plan, plan_smem, tile_rows, tile_cols, w_first, w_second = take(11)
    values_sem, x_sem, plan_sem, out_sem, small_sem, spread_send, share_recv, sum_send = take(8)
    panels = [take(2), take(2)]
    row, col = lax.axis_index("row"), lax.axis_index("col")
    spreads = [
        [
            [
                Spread(unit, panels[layer][f], take(1) + [spread_send, share_recv.at[layer, f]], row, col)
                for unit in SPREADS[layer]
            ]
            for f in range(2)
        ]
        for layer in range(2)
    ]
    sums = [
        [Sum(unit, part, *take(2), take(2) + [sum_send.at[layer]], row, col) for unit in UNITS[layer]]
        for layer in range(2)
    ]

    first_spread = spreads[0][0][0]
    first_sum = sums[0][0]
    partners = [(step, col) for step in first_spread.steps] + [(first_spread.mate, col)]
    for half, way in Sum.both:
        first, second = first_sum.spot(half)
        partners.append((row, first_sum.place(half, first_sum.step(first, way), second)))
    barrier = pltpu.get_barrier_semaphore()
    for to_row, to_col in partners:
        pl.semaphore_signal(barrier, inc=1, device_id=(to_row, to_col), device_id_type=MESH)

    loads = [
        pltpu.make_async_copy(
            x.at[:, :, pl.ds(f * WIDE, WIDE)], panels[0][f].at[pl.ds(row * BLOCK_TILES, BLOCK_TILES)], x_sem.at[f]
        )
        for f in range(2)
    ]
    small = [
        pltpu.make_async_copy(source, target, small_sem.at[i])
        for i, (source, target) in enumerate(
            ((rows_hbm, tile_rows), (cols_hbm, tile_cols), (w_first_hbm, w_first), (w_second_hbm, w_second))
        )
    ]
    for copy in [loads[0]] + small[:2] + [loads[1]] + small[2:]:
        copy.start()
    values_load = pltpu.make_async_copy(values_hbm.at[0, 0], values, values_sem)
    values_load.start()
    pl.semaphore_wait(barrier, len(partners))
    loads[0].wait()
    spreads[0][0][0].own()
    for copy in small:
        copy.wait()

    lane = lax.broadcasted_iota(jnp.int32, (1, SLOTS), 1)
    key = jnp.where(lane < tile_count[0, 0], tile_rows[...] * 64 + tile_cols[...], lane + 8192)
    across = jnp.broadcast_to(key.astype(jnp.float32), (SLOTS, SLOTS))
    down = jnp.transpose(across)
    rank = jnp.sum(jnp.where(across < down, 1.0, 0.0), axis=1, keepdims=True)
    lanes = lax.broadcasted_iota(jnp.int32, (SLOTS, SLOTS), 1).astype(jnp.float32)
    slots = lax.broadcasted_iota(jnp.int32, (SLOTS, SLOTS), 0).astype(jnp.float32)

    def pick(condition, what):
        return jnp.sum(jnp.where(condition, what, 0.0), axis=0, keepdims=True).astype(jnp.int32)

    order = pick(rank == lanes, slots)
    ordered = pick(rank == lanes, down)
    before = pick(rank == lanes - 1.0, down)
    ends = pick(down < (lanes + 1.0) * 64.0, 1.0)
    starts = pick(down < lanes * 64.0, 1.0)
    same = jnp.where(jnp.right_shift(ordered, 6) == jnp.right_shift(before, 6), 1, 0)
    run_of = jnp.where(ends == starts, SLOTS, ends - 1)
    rest = jnp.zeros((4, SLOTS), jnp.int32)
    plan[...] = jnp.concatenate([order, jnp.bitwise_and(ordered, 63), run_of, same, rest], axis=0)
    for f in range(2):
        runs[f, SLOTS] = jnp.zeros((TILE, WIDE), BF16)
    plan_copy = pltpu.make_async_copy(plan, plan_smem, plan_sem)
    plan_copy.start()

    def multiply(panel, f, first, last, total):
        def block(it, total):
            for u in range(UNROLL):
                at = it * UNROLL + u
                slot = jnp.clip(plan_smem[0, at], 0, SLOTS - 1)
                column = jnp.clip(plan_smem[1, at], 0, 63)
                keep = jnp.where(plan_smem[3, at] == 1, 1.0, 0.0)
                total = total * keep + jnp.dot(values[slot], panel[column], preferred_element_type=jnp.float32)
                runs[f, at] = total.astype(BF16)
            return total

        return lax.fori_loop(first // UNROLL, last // UNROLL, block, total)

    empty = jnp.zeros((TILE, WIDE), jnp.float32)

    def fill(unit, half, first):
        tiles = unit.rows // 2 // TILE
        base = unit.r0 // TILE + half * tiles

        @pl.loop(0, SIDE, unroll=SIDE if tiles == 1 else 1)
        def _(second):
            up, across = (second, first) if half == 0 else (first, second)
            for t in range(base, base + tiles):
                run = jnp.clip(plan_smem[2, (up * SIDE + across) * BLOCK_TILES + t], 0, SLOTS)
                for f in range(unit.f0, unit.f0 + unit.nf):
                    part[f, up, across, pl.ds(t * TILE, TILE)] = runs[f, run]

    def weigh(unit, w, store):
        @pl.loop(0, unit.rows // TILE, unroll=unit.rows // TILE)
        def _(i):
            t = unit.r0 // TILE + i
            lines = pl.ds(pl.multiple_of(t * TILE, TILE), TILE)
            both = jnp.concatenate([summed[0, lines], summed[1, lines]], axis=1)
            product = jnp.dot(both, w[...], preferred_element_type=jnp.float32)
            store(t, jnp.maximum(product, 0.0).astype(BF16))

    def keep_hidden(t, block):
        for f in range(2):
            panels[1][f][row * BLOCK_TILES + t] = block[:, f * WIDE : (f + 1) * WIDE]

    def write(t):
        lines = pl.ds(pl.multiple_of(t * TILE, TILE), TILE)
        return pltpu.make_async_copy(staged.at[lines], out.at[lines], out_sem)

    def keep_output(t, block):
        staged[pl.ds(pl.multiple_of(t * TILE, TILE), TILE)] = block
        write(t).start()

    def shared(layer, f):
        await_bytes(panels[layer][f].at[pl.ds(0, 32)], share_recv.at[layer, f])

    (a,), (b,) = spreads[0]
    a0, a1, b0, b1, b2, b3 = sums[0]
    (g0, g1, g2, g3), (h0, h1, h2, h3) = spreads[1]
    d, e0, e1 = sums[1]
    a.onward(0)
    loads[1].wait()
    b.own()
    a.onward(1)
    a.onward(2)
    shared(0, 0)
    plan_copy.wait()
    values_load.wait()
    total = multiply(panels[0][0], 0, 0, 128, empty)
    total = multiply(panels[0][0], 0, 128, 256, total)
    a0.open(fill)
    b.onward(0)
    b.onward(1)
    a0.merge1()
    b.onward(2)
    shared(0, 1)
    a1.open(fill)
    total = multiply(panels[0][1], 1, 0, 128, empty)
    total = multiply(panels[0][1], 1, 128, 256, total)
    b1.open(fill)
    a0.turn()
    b0.open(fill)
    b1.merge1()
    b0.merge1()
    b2.open(fill)
    b0.turn()
    a0.merge2()
    a1.merge1()
    b0.merge2()
    b1.turn()
    a0.close(summed)
    b3.open(fill)
    b0.close(summed)
    b1.merge2()
    weigh(b0, w_first, keep_hidden)
    h0.own()
    b2.merge1()
    b3.merge1()
    a1.turn()
    g0.own()
    b1.close(summed)
    weigh(b1, w_first, keep_hidden)
    g1.own()
    b2.turn()
    h1.own()
    b3.turn()
    a1.merge2()
    g0.onward(0)
    b2.merge2()
    b3.merge2()
    h1.onward(0)
    h1.onward(1)
    g1.onward(0)
    a1.close(summed)
    b2.close(summed)
    weigh(b2, w_first, keep_hidden)
    g0.onward(1)
    g1.onward(1)
    g2.own()
    b3.close(summed)
    weigh(b3, w_first, keep_hidden)
    g3.own()
    h2.own()
    g2.onward(0)
    g3.onward(0)
    h3.own()
    h0.onward(0)
    g1.onward(2)
    g2.onward(1)
    g0.onward(2)
    g3.onward(1)
    g2.onward(2)
    h1.onward(2)
    h0.onward(1)
    h2.onward(0)
    g3.onward(2)
    h3.onward(0)
    h2.onward(1)
    shared(1, 0)
    await_bytes(values.at[pl.ds(0, 240)], sum_send.at[0])

    total = multiply(panels[1][0], 0, 0, 128, empty)
    h2.onward(2)
    h0.onward(2)
    h3.onward(1)
    total = multiply(panels[1][0], 0, 128, 256, total)
    h3.onward(2)
    d.open(fill)
    shared(1, 1)
    total = multiply(panels[1][1], 1, 0, 128, empty)
    d.merge1()
    total = multiply(panels[1][1], 1, 128, 256, total)
    e1.open(fill)
    e0.open(fill)
    e1.merge1()
    e0.merge1()
    d.turn()
    e1.turn()
    e0.turn()
    d.merge2()
    e1.merge2()
    e0.merge2()
    d.close(summed)
    e1.close(summed)
    weigh(e1, w_second, keep_output)
    e0.close(summed)
    weigh(e0, w_second, keep_output)
    await_bytes(values.at[pl.ds(0, 224)], spread_send)
    await_bytes(values.at[pl.ds(0, 240)], sum_send.at[1])
    await_bytes(staged, out_sem)


def both_layers(x, values, rows, cols, count, w_first, w_second):
    smem, hbm = pl.BlockSpec(memory_space=pltpu.SMEM), pl.BlockSpec(memory_space=pl.ANY)
    dma = pltpu.SemaphoreType.DMA
    scratch = [
        pltpu.VMEM((SLOTS, TILE, TILE), BF16),
        pltpu.VMEM((2, SLOTS + 1, TILE, WIDE), BF16),
        pltpu.VMEM((2, SIDE, SIDE, NODES, WIDE), BF16),
        pltpu.VMEM((2, NODES, WIDE), BF16),
        pltpu.VMEM((NODES, F), BF16),
        pltpu.VMEM((8, SLOTS), jnp.int32),
        pltpu.SMEM((8, SLOTS), jnp.int32),
        pltpu.VMEM((1, SLOTS), jnp.int32),
        pltpu.VMEM((1, SLOTS), jnp.int32),
        pltpu.VMEM((F, F), BF16),
        pltpu.VMEM((F, F), BF16),
        dma,
        dma((2,)),
        dma,
        dma,
        dma((4,)),
        dma,
        dma((2, 2)),
        dma((2,)),
    ]
    scratch += [pltpu.VMEM((64, TILE, WIDE), BF16)] * 4
    for layer in range(2):
        for _ in SPREADS[layer] * 2:
            scratch += [dma((3,))]
    for layer in range(2):
        for _, nf, _, rows_of in UNITS[layer]:
            scratch += [
                pltpu.VMEM((2, 2, 3, nf, SIDE, rows_of // 4, WIDE), BF16),
                pltpu.VMEM((2, 2, 3, nf, rows_of // 4, WIDE), BF16),
                dma((2, 2)), dma((2, 2)),
            ]
    return pl.pallas_call(
        kernel,
        out_shape=jax.ShapeDtypeStruct((NODES, F), BF16),
        in_specs=[hbm, hbm, hbm, hbm, smem, hbm, hbm],
        out_specs=hbm,
        scratch_shapes=scratch,
        compiler_params=pltpu.CompilerParams(
            collective_id=0, has_side_effects=True, vmem_limit_bytes=67043328
        ),
        name="layers",
    )(x, values, rows, cols, count, w_first, w_second)


def shards(features, tile_values, tile_rows, tile_cols, tile_count, w_first, w_second):
    return both_layers(
        features.reshape(BLOCK_TILES, TILE, F), tile_values, tile_rows[0], tile_cols[0], tile_count, w_first, w_second
    )


def solution(mesh):
    return jax.shard_map(
        shards,
        mesh=mesh,
        in_specs=(
            P(("row", "col"), None),
            P("row", "col", None, None, None),
            P("row", "col", None),
            P("row", "col", None),
            P("row", "col"),
            P(),
            P(),
        ),
        out_specs=P(("row", "col"), None),
        check_vma=False,
    )
```

```python
import jax
import jax.numpy as jnp
from jax import lax
from jax.experimental import pallas as pl
from jax.experimental.pallas import tpu as pltpu
from jax.sharding import PartitionSpec as P

MESH = pl.DeviceIdType.MESH
F = 256
WIDE = 128
TILE = 128
SLOTS = 256
NODES = 1024
SIDE = 4
BLOCK_TILES = NODES // TILE
UNROLL = 128
FAR, RAW, MERGED = 0, 1, 2
BF16 = jnp.bfloat16

UNITS = (
    ((0, 1, 0, 512), (0, 1, 512, 512), (1, 1, 0, 256), (1, 1, 256, 256), (1, 1, 512, 256), (1, 1, 768, 256)),
    ((0, 1, 0, 1024), (1, 1, 0, 512), (1, 1, 512, 512)),
)
SPREADS = (((0, 8),), ((0, 2), (2, 2), (4, 2), (6, 2)))


LAST = (1, 0, SPREADS[1][-1])


def remote(src, dst, send, recv, row, col):
    return pltpu.make_async_remote_copy(
        src_ref=src, dst_ref=dst, send_sem=send, recv_sem=recv, device_id=(row, col), device_id_type=MESH
    )


def await_bytes(sized, sem):
    pltpu.make_async_copy(sized, sized, sem).wait()


class Spread:
    def __init__(self, unit, panel, sems, row, col, pair=False):
        self.t0, self.tiles = unit
        self.pair = pair
        self.panel, self.row, self.col = panel, row, col
        self.recv, self.send, self.mate_recv = sems
        self.z, self.core = row // 2, row % 2
        self.mate = self.z * 2 + 1 - self.core
        self.steps = ((self.z + 1) % SIDE * 2 + self.core, (self.z + 3) % SIDE * 2 + self.core)
        self.across = tuple(step + 1 - 2 * self.core for step in self.steps)
        self.groups = (((3, 0), (1, 1)), ((3, 1), (1, 0)), ((2, 0), (2, 1)))

    def at(self, distance, core):
        return (self.z + distance) % SIDE * 2 + core

    def part(self, block, which):
        half = self.tiles // 2
        return self.panel.at[pl.ds(block * BLOCK_TILES + self.t0 + which * half, half)]

    def sized(self, tiles):
        return self.panel.at[pl.ds(0, tiles)]

    def hop(self, way, order, block, which):
        piece = self.part(block, which)
        remote(piece, piece, self.send, self.recv.at[order], self.steps[way], self.col).start()

    def share(self, block, which):
        piece = self.part(block, which)
        remote(piece, piece, self.send, self.mate_recv, self.mate, self.col).start()

    def own(self):
        for order in range(2):
            for way in range(2):
                self.hop(way, order, self.row, way ^ order)
        for which in range(2):
            self.share(self.row, which)

    def onward(self, order):
        await_bytes(self.sized(self.tiles), self.recv.at[order])
        for way in range(2):
            distance, which = self.groups[order][way]
            block = self.at(distance, self.core)
            if order == 0:
                self.hop(way, 2, block, which)
                if self.pair:
                    piece = self.part(block, which)
                    remote(piece, piece, self.send, self.mate_recv, self.across[way], self.col).start()
            if order < 2 or not self.pair:
                self.share(block, which)


class Sum:
    def __init__(self, unit, part, got1, got2, sems, row, col):
        self.f0, self.nf, self.r0, self.rows = unit
        self.quarter = self.rows // 4
        self.part, self.got1, self.got2 = part, got1, got2
        self.recv1, self.recv2, self.send = sems
        self.row = row
        self.y, self.x = col // SIDE, col % SIDE

    def spot(self, half):
        return (self.x, self.y) if half == 0 else (self.y, self.x)

    def step(self, at, way):
        return (at + (1 if way == 0 else SIDE - 1)) % SIDE

    def place(self, half, first, second):
        return second * SIDE + first if half == 0 else first * SIDE + second

    def lines(self, half, h):
        return pl.ds(self.r0 + (2 * half + h) * self.quarter, self.quarter)

    def group(self, half, first, h):
        halves = pl.ds(self.f0, self.nf)
        if half == 0:
            return self.part.at[halves, :, first, self.lines(half, h)]
        return self.part.at[halves, first, :, self.lines(half, h)]

    def single(self, half, second, h):
        halves = pl.ds(self.f0, self.nf)
        first = self.spot(half)[0]
        if half == 0:
            return self.part.at[halves, second, first, self.lines(half, h)]
        return self.part.at[halves, first, second, self.lines(half, h)]

    def hop1(self, half, way, kind):
        first, second = self.spot(half)
        if kind == FAR:
            src = self.group(half, (first + 2) % SIDE, way)
        elif kind == RAW:
            src = self.group(half, self.step(first, way), 1 - way)
        else:
            src = self.group(half, self.step(first, way), way)
        remote(
            src, self.got1.at[half, way, kind], self.send, self.recv1.at[half, min(kind, 1)],
            self.row, self.place(half, self.step(first, way), second),
        ).start()

    def hop2(self, half, way, kind):
        first, second = self.spot(half)
        if kind == FAR:
            src = self.single(half, (second + 2) % SIDE, way)
        elif kind == RAW:
            src = self.single(half, self.step(second, way), 1 - way)
        else:
            src = self.single(half, self.step(second, way), way)
        remote(
            src, self.got2.at[half, way, kind], self.send, self.recv2.at[half, min(kind, 1)],
            self.row, self.place(half, first, self.step(second, way)),
        ).start()

    def arrive(self, got, recv, half, kind):
        kinds = pl.ds(0, 1) if kind == FAR else pl.ds(1, 2)
        await_bytes(got.at[half, :, kinds], recv.at[half, kind])

    both = tuple((half, way) for half in range(2) for way in range(2))

    def open(self, fill):
        for half in range(2):
            fill(self, half, (self.spot(half)[0] + 2) % SIDE)
        for half, way in self.both:
            self.hop1(half, way, FAR)
        for way in range(2):
            for half in range(2):
                fill(self, half, self.step(self.spot(half)[0], way))
        for half, way in self.both:
            self.hop1(half, way, RAW)
        for half in range(2):
            fill(self, half, self.spot(half)[0])

    def merge1(self):
        for half, way in self.both:
            if way == 0:
                self.arrive(self.got1, self.recv1, half, FAR)
            mine = self.group(half, self.step(self.spot(half)[0], way), way)
            got = self.got1.at[half, way, FAR]

            @pl.loop(0, self.nf * SIDE)
            def _(i):
                f, j = i // SIDE, i % SIDE
                mine[f, j] = (mine[f, j].astype(jnp.float32) + got[f, j].astype(jnp.float32)).astype(BF16)

            self.hop1(half, way, MERGED)

    def turn(self):
        for half in range(2):
            second = self.spot(half)[1]
            self.arrive(self.got1, self.recv1, half, RAW)
            for h in range(2):
                mine = self.group(half, self.spot(half)[0], h)
                one, two = self.got1.at[half, h, MERGED], self.got1.at[half, 1 - h, RAW]

                @pl.loop(0, self.nf * (SIDE - 1))
                def _(i):
                    f, j = i // (SIDE - 1), (second + 1 + i % (SIDE - 1)) % SIDE
                    total = mine[f, j].astype(jnp.float32) + one[f, j].astype(jnp.float32)
                    mine[f, j] = (total + two[f, j].astype(jnp.float32)).astype(BF16)

            for way in range(2):
                self.hop2(half, way, FAR)
            for way in range(2):
                self.hop2(half, way, RAW)

    def merge2(self):
        for half, way in self.both:
            if way == 0:
                self.arrive(self.got2, self.recv2, half, FAR)
            mine = self.single(half, self.step(self.spot(half)[1], way), way)
            got = self.got2.at[half, way, FAR]
            for f in range(self.nf):
                mine[f] = (mine[f].astype(jnp.float32) + got[f].astype(jnp.float32)).astype(BF16)
            self.hop2(half, way, MERGED)

    def close(self, summed):
        for half in range(2):
            second = self.spot(half)[1]
            self.arrive(self.got2, self.recv2, half, RAW)
            for h in range(2):
                mine = self.single(half, second, h)
                for f in range(self.nf):
                    total = mine[f].astype(jnp.float32)
                    total = total + self.got1[half, h, MERGED, f, second].astype(jnp.float32)
                    total = total + self.got1[half, 1 - h, RAW, f, second].astype(jnp.float32)
                    total = total + self.got2[half, h, MERGED, f].astype(jnp.float32)
                    total = total + self.got2[half, 1 - h, RAW, f].astype(jnp.float32)
                    summed[self.f0 + f, self.lines(half, h)] = total.astype(BF16)


def kernel(x, values_hbm, rows_hbm, cols_hbm, tile_count, w_first_hbm, w_second_hbm, out, *scratch):
    scratch = list(scratch)

    def take(number):
        taken = scratch[:number]
        del scratch[:number]
        return taken

    values, runs, part, summed, staged, plan, plan_smem, tile_rows, tile_cols, w_first, w_second = take(11)
    values_sem, x_sem, plan_sem, out_sem, small_sem, spread_send, share_recv, sum_send = take(8)
    panels = [take(2), take(2)]
    row, col = lax.axis_index("row"), lax.axis_index("col")
    spreads = [
        [
            [
                Spread(unit, panels[layer][f], take(1) + [spread_send, share_recv.at[layer, f]], row, col, (layer, f, unit) == LAST)
                for unit in SPREADS[layer]
            ]
            for f in range(2)
        ]
        for layer in range(2)
    ]
    sums = [
        [Sum(unit, part, *take(2), take(2) + [sum_send.at[layer]], row, col) for unit in UNITS[layer]]
        for layer in range(2)
    ]

    first_spread = spreads[0][0][0]
    first_sum = sums[0][0]
    partners = [(step, col) for step in first_spread.steps + first_spread.across + (first_spread.mate,)]
    for half, way in Sum.both:
        first, second = first_sum.spot(half)
        partners.append((row, first_sum.place(half, first_sum.step(first, way), second)))
    barrier = pltpu.get_barrier_semaphore()
    for to_row, to_col in partners:
        pl.semaphore_signal(barrier, inc=1, device_id=(to_row, to_col), device_id_type=MESH)

    loads = [
        pltpu.make_async_copy(
            x.at[:, :, pl.ds(f * WIDE, WIDE)], panels[0][f].at[pl.ds(row * BLOCK_TILES, BLOCK_TILES)], x_sem.at[f]
        )
        for f in range(2)
    ]
    small = [
        pltpu.make_async_copy(source, target, small_sem.at[i])
        for i, (source, target) in enumerate(
            ((rows_hbm, tile_rows), (cols_hbm, tile_cols), (w_first_hbm, w_first), (w_second_hbm, w_second))
        )
    ]
    for copy in [loads[0]] + small[:2] + [loads[1]] + small[2:]:
        copy.start()
    values_load = pltpu.make_async_copy(values_hbm.at[0, 0], values, values_sem)
    values_load.start()
    pl.semaphore_wait(barrier, len(partners))
    loads[0].wait()
    spreads[0][0][0].own()
    for copy in small:
        copy.wait()

    lane = lax.broadcasted_iota(jnp.int32, (1, SLOTS), 1)
    key = jnp.where(lane < tile_count[0, 0], tile_rows[...] * 64 + tile_cols[...], lane + 8192)
    across = jnp.broadcast_to(key.astype(jnp.float32), (SLOTS, SLOTS))
    down = jnp.transpose(across)
    rank = jnp.sum(jnp.where(across < down, 1.0, 0.0), axis=1, keepdims=True)
    lanes = lax.broadcasted_iota(jnp.int32, (SLOTS, SLOTS), 1).astype(jnp.float32)
    slots = lax.broadcasted_iota(jnp.int32, (SLOTS, SLOTS), 0).astype(jnp.float32)

    def pick(condition, what):
        return jnp.sum(jnp.where(condition, what, 0.0), axis=0, keepdims=True).astype(jnp.int32)

    order = pick(rank == lanes, slots)
    ordered = pick(rank == lanes, down)
    before = pick(rank == lanes - 1.0, down)
    ends = pick(down < (lanes + 1.0) * 64.0, 1.0)
    starts = pick(down < lanes * 64.0, 1.0)
    same = jnp.where(jnp.right_shift(ordered, 6) == jnp.right_shift(before, 6), 1, 0)
    run_of = jnp.where(ends == starts, SLOTS, ends - 1)
    rest = jnp.zeros((4, SLOTS), jnp.int32)
    plan[...] = jnp.concatenate([order, jnp.bitwise_and(ordered, 63), run_of, same, rest], axis=0)
    for f in range(2):
        runs[f, SLOTS] = jnp.zeros((TILE, WIDE), BF16)
    plan_copy = pltpu.make_async_copy(plan, plan_smem, plan_sem)
    plan_copy.start()

    def multiply(panel, f, first, last, total):
        def block(it, total):
            for u in range(UNROLL):
                at = it * UNROLL + u
                slot = jnp.clip(plan_smem[0, at], 0, SLOTS - 1)
                column = jnp.clip(plan_smem[1, at], 0, 63)
                keep = jnp.where(plan_smem[3, at] == 1, 1.0, 0.0)
                total = total * keep + jnp.dot(values[slot], panel[column], preferred_element_type=jnp.float32)
                runs[f, at] = total.astype(BF16)
            return total

        return lax.fori_loop(first // UNROLL, last // UNROLL, block, total)

    empty = jnp.zeros((TILE, WIDE), jnp.float32)

    def fill(unit, half, first):
        tiles = unit.rows // 2 // TILE
        base = unit.r0 // TILE + half * tiles

        @pl.loop(0, SIDE, unroll=SIDE if tiles == 1 else 1)
        def _(second):
            up, across = (second, first) if half == 0 else (first, second)
            for t in range(base, base + tiles):
                run = jnp.clip(plan_smem[2, (up * SIDE + across) * BLOCK_TILES + t], 0, SLOTS)
                for f in range(unit.f0, unit.f0 + unit.nf):
                    part[f, up, across, pl.ds(t * TILE, TILE)] = runs[f, run]

    def weigh(unit, w, store):
        @pl.loop(0, unit.rows // TILE, unroll=unit.rows // TILE)
        def _(i):
            t = unit.r0 // TILE + i
            lines = pl.ds(pl.multiple_of(t * TILE, TILE), TILE)
            both = jnp.concatenate([summed[0, lines], summed[1, lines]], axis=1)
            product = jnp.dot(both, w[...], preferred_element_type=jnp.float32)
            store(t, jnp.maximum(product, 0.0).astype(BF16))

    def keep_hidden(t, block):
        for f in range(2):
            panels[1][f][row * BLOCK_TILES + t] = block[:, f * WIDE : (f + 1) * WIDE]

    def write(t):
        lines = pl.ds(pl.multiple_of(t * TILE, TILE), TILE)
        return pltpu.make_async_copy(staged.at[lines], out.at[lines], out_sem)

    def keep_output(t, block):
        staged[pl.ds(pl.multiple_of(t * TILE, TILE), TILE)] = block
        write(t).start()

    def shared(layer, f):
        await_bytes(panels[layer][f].at[pl.ds(0, 32)], share_recv.at[layer, f])

    (a,), (b,) = spreads[0]
    a0, a1, b0, b1, b2, b3 = sums[0]
    (g0, g1, g2, g3), (h0, h1, h2, h3) = spreads[1]
    d, e0, e1 = sums[1]
    a.onward(0)
    loads[1].wait()
    b.own()
    a.onward(1)
    a.onward(2)
    shared(0, 0)
    plan_copy.wait()
    values_load.wait()
    total = multiply(panels[0][0], 0, 0, 128, empty)
    total = multiply(panels[0][0], 0, 128, 256, total)
    a0.open(fill)
    b.onward(0)
    b.onward(1)
    a0.merge1()
    b.onward(2)
    shared(0, 1)
    a1.open(fill)
    total = multiply(panels[0][1], 1, 0, 128, empty)
    total = multiply(panels[0][1], 1, 128, 256, total)
    b1.open(fill)
    a0.turn()
    b0.open(fill)
    b1.merge1()
    b0.merge1()
    b2.open(fill)
    b0.turn()
    a0.merge2()
    a1.merge1()
    b0.merge2()
    b1.turn()
    a0.close(summed)
    b3.open(fill)
    b0.close(summed)
    b1.merge2()
    weigh(b0, w_first, keep_hidden)
    h0.own()
    b2.merge1()
    b3.merge1()
    a1.turn()
    g0.own()
    b1.close(summed)
    weigh(b1, w_first, keep_hidden)
    g1.own()
    b2.turn()
    h1.own()
    b3.turn()
    a1.merge2()
    g0.onward(0)
    b2.merge2()
    b3.merge2()
    h1.onward(0)
    h1.onward(1)
    g1.onward(0)
    a1.close(summed)
    b2.close(summed)
    weigh(b2, w_first, keep_hidden)
    g0.onward(1)
    g1.onward(1)
    g2.own()
    b3.close(summed)
    weigh(b3, w_first, keep_hidden)
    g3.own()
    g2.onward(0)
    g3.onward(0)
    h2.own()
    h3.own()
    h0.onward(0)
    g1.onward(2)
    g2.onward(1)
    g0.onward(2)
    g3.onward(1)
    g2.onward(2)
    h1.onward(2)
    h0.onward(1)
    h2.onward(0)
    g3.onward(2)
    h3.onward(0)
    h2.onward(1)
    shared(1, 0)
    await_bytes(values.at[pl.ds(0, 240)], sum_send.at[0])

    total = multiply(panels[1][0], 0, 0, 128, empty)
    h2.onward(2)
    h0.onward(2)
    h3.onward(1)
    total = multiply(panels[1][0], 0, 128, 256, total)
    h3.onward(2)
    d.open(fill)
    shared(1, 1)
    total = multiply(panels[1][1], 1, 0, 128, empty)
    d.merge1()
    total = multiply(panels[1][1], 1, 128, 256, total)
    e1.open(fill)
    e0.open(fill)
    e1.merge1()
    e0.merge1()
    d.turn()
    e1.turn()
    e0.turn()
    d.merge2()
    e1.merge2()
    e0.merge2()
    d.close(summed)
    e1.close(summed)
    weigh(e1, w_second, keep_output)
    e0.close(summed)
    weigh(e0, w_second, keep_output)
    await_bytes(values.at[pl.ds(0, 224)], spread_send)
    await_bytes(values.at[pl.ds(0, 240)], sum_send.at[1])
    await_bytes(staged, out_sem)


def both_layers(x, values, rows, cols, count, w_first, w_second):
    smem, hbm = pl.BlockSpec(memory_space=pltpu.SMEM), pl.BlockSpec(memory_space=pl.ANY)
    dma = pltpu.SemaphoreType.DMA
    scratch = [
        pltpu.VMEM((SLOTS, TILE, TILE), BF16),
        pltpu.VMEM((2, SLOTS + 1, TILE, WIDE), BF16),
        pltpu.VMEM((2, SIDE, SIDE, NODES, WIDE), BF16),
        pltpu.VMEM((2, NODES, WIDE), BF16),
        pltpu.VMEM((NODES, F), BF16),
        pltpu.VMEM((8, SLOTS), jnp.int32),
        pltpu.SMEM((8, SLOTS), jnp.int32),
        pltpu.VMEM((1, SLOTS), jnp.int32),
        pltpu.VMEM((1, SLOTS), jnp.int32),
        pltpu.VMEM((F, F), BF16),
        pltpu.VMEM((F, F), BF16),
        dma,
        dma((2,)),
        dma,
        dma,
        dma((4,)),
        dma,
        dma((2, 2)),
        dma((2,)),
    ]
    scratch += [pltpu.VMEM((64, TILE, WIDE), BF16)] * 4
    for layer in range(2):
        for _ in SPREADS[layer] * 2:
            scratch += [dma((3,))]
    for layer in range(2):
        for _, nf, _, rows_of in UNITS[layer]:
            scratch += [
                pltpu.VMEM((2, 2, 3, nf, SIDE, rows_of // 4, WIDE), BF16),
                pltpu.VMEM((2, 2, 3, nf, rows_of // 4, WIDE), BF16),
                dma((2, 2)), dma((2, 2)),
            ]
    return pl.pallas_call(
        kernel,
        out_shape=jax.ShapeDtypeStruct((NODES, F), BF16),
        in_specs=[hbm, hbm, hbm, hbm, smem, hbm, hbm],
        out_specs=hbm,
        scratch_shapes=scratch,
        compiler_params=pltpu.CompilerParams(
            collective_id=0, has_side_effects=True, vmem_limit_bytes=67043328
        ),
        name="layers",
    )(x, values, rows, cols, count, w_first, w_second)


def shards(features, tile_values, tile_rows, tile_cols, tile_count, w_first, w_second):
    return both_layers(
        features.reshape(BLOCK_TILES, TILE, F), tile_values, tile_rows[0], tile_cols[0], tile_count, w_first, w_second
    )


def solution(mesh):
    return jax.shard_map(
        shards,
        mesh=mesh,
        in_specs=(
            P(("row", "col"), None),
            P("row", "col", None, None, None),
            P("row", "col", None),
            P("row", "col", None),
            P("row", "col"),
            P(),
            P(),
        ),
        out_specs=P(("row", "col"), None),
        check_vma=False,
    )
```

```python
import jax
import jax.numpy as jnp
from jax import lax
from jax.experimental import pallas as pl
from jax.experimental.pallas import tpu as pltpu
from jax.sharding import PartitionSpec as P

MESH = pl.DeviceIdType.MESH
F = 256
WIDE = 128
TILE = 128
SLOTS = 256
NODES = 1024
SIDE = 4
BLOCK_TILES = NODES // TILE
FAR, RAW, MERGED = 0, 1, 2
BF16 = jnp.bfloat16

UNITS = (
    ((0, 1, 0, 512), (0, 1, 512, 512), (1, 1, 0, 256), (1, 1, 256, 256), (1, 1, 512, 256), (1, 1, 768, 256)),
    ((0, 1, 0, 1024), (1, 1, 0, 512), (1, 1, 512, 512)),
)
SPREADS = (((0, 8),), ((0, 2), (2, 2), (4, 2), (6, 2)))


def remote(src, dst, send, recv, row, col):
    return pltpu.make_async_remote_copy(
        src_ref=src, dst_ref=dst, send_sem=send, recv_sem=recv, device_id=(row, col), device_id_type=MESH
    )


def await_bytes(sized, sem):
    pltpu.make_async_copy(sized, sized, sem).wait()


class Spread:
    def __init__(self, unit, panel, sems, row, col):
        self.t0, self.tiles = unit
        self.panel, self.row, self.col = panel, row, col
        self.recv, self.send, self.mate_recv = sems
        self.z, self.core = row // 2, row % 2
        self.mate = self.z * 2 + 1 - self.core
        self.steps = ((self.z + 1) % SIDE * 2 + self.core, (self.z + 3) % SIDE * 2 + self.core)
        self.groups = (((3, 0), (1, 1)), ((3, 1), (1, 0)), ((2, 0), (2, 1)))

    def at(self, distance, core):
        return (self.z + distance) % SIDE * 2 + core

    def part(self, block, which):
        half = self.tiles // 2
        return self.panel.at[pl.ds(block * BLOCK_TILES + self.t0 + which * half, half)]

    def sized(self, tiles):
        return self.panel.at[pl.ds(0, tiles)]

    def hop(self, way, order, block, which):
        piece = self.part(block, which)
        remote(piece, piece, self.send, self.recv.at[order], self.steps[way], self.col).start()

    def share(self, block, which):
        piece = self.part(block, which)
        remote(piece, piece, self.send, self.mate_recv, self.mate, self.col).start()

    def own(self):
        for order in range(2):
            for way in range(2):
                self.hop(way, order, self.row, way ^ order)
        for which in range(2):
            self.share(self.row, which)

    def onward(self, order):
        await_bytes(self.sized(self.tiles), self.recv.at[order])
        for way in range(2):
            distance, which = self.groups[order][way]
            block = self.at(distance, self.core)
            if order == 0:
                self.hop(way, 2, block, which)
            self.share(block, which)


class Sum:
    def __init__(self, unit, part, got1, got2, sems, row, col):
        self.f0, self.nf, self.r0, self.rows = unit
        self.quarter = self.rows // 4
        self.part, self.got1, self.got2 = part, got1, got2
        self.recv1, self.recv2, self.send = sems
        self.row = row
        self.y, self.x = col // SIDE, col % SIDE

    def spot(self, half):
        return (self.x, self.y) if half == 0 else (self.y, self.x)

    def step(self, at, way):
        return (at + (1 if way == 0 else SIDE - 1)) % SIDE

    def place(self, half, first, second):
        return second * SIDE + first if half == 0 else first * SIDE + second

    def lines(self, half, h):
        return pl.ds(self.r0 + (2 * half + h) * self.quarter, self.quarter)

    def group(self, half, first, h):
        halves = pl.ds(self.f0, self.nf)
        if half == 0:
            return self.part.at[halves, :, first, self.lines(half, h)]
        return self.part.at[halves, first, :, self.lines(half, h)]

    def single(self, half, second, h):
        halves = pl.ds(self.f0, self.nf)
        first = self.spot(half)[0]
        if half == 0:
            return self.part.at[halves, second, first, self.lines(half, h)]
        return self.part.at[halves, first, second, self.lines(half, h)]

    def hop1(self, half, way, kind):
        first, second = self.spot(half)
        if kind == FAR:
            src = self.group(half, (first + 2) % SIDE, way)
        elif kind == RAW:
            src = self.group(half, self.step(first, way), 1 - way)
        else:
            src = self.group(half, self.step(first, way), way)
        remote(
            src, self.got1.at[half, way, kind], self.send, self.recv1.at[half, min(kind, 1)],
            self.row, self.place(half, self.step(first, way), second),
        ).start()

    def hop2(self, half, way, kind):
        first, second = self.spot(half)
        if kind == FAR:
            src = self.single(half, (second + 2) % SIDE, way)
        elif kind == RAW:
            src = self.single(half, self.step(second, way), 1 - way)
        else:
            src = self.single(half, self.step(second, way), way)
        remote(
            src, self.got2.at[half, way, kind], self.send, self.recv2.at[half, min(kind, 1)],
            self.row, self.place(half, first, self.step(second, way)),
        ).start()

    def arrive(self, got, recv, half, kind):
        kinds = pl.ds(0, 1) if kind == FAR else pl.ds(1, 2)
        await_bytes(got.at[half, :, kinds], recv.at[half, kind])

    both = tuple((half, way) for half in range(2) for way in range(2))

    def open(self, fill):
        for half in range(2):
            fill(self, half, (self.spot(half)[0] + 2) % SIDE)
        for half, way in self.both:
            self.hop1(half, way, FAR)
        for way in range(2):
            for half in range(2):
                fill(self, half, self.step(self.spot(half)[0], way))
        for half, way in self.both:
            self.hop1(half, way, RAW)
        for half in range(2):
            fill(self, half, self.spot(half)[0])

    def merge1(self):
        for half, way in self.both:
            if way == 0:
                self.arrive(self.got1, self.recv1, half, FAR)
            mine = self.group(half, self.step(self.spot(half)[0], way), way)
            got = self.got1.at[half, way, FAR]

            @pl.loop(0, self.nf * SIDE)
            def _(i):
                f, j = i // SIDE, i % SIDE
                mine[f, j] = (mine[f, j].astype(jnp.float32) + got[f, j].astype(jnp.float32)).astype(BF16)

            self.hop1(half, way, MERGED)

    def turn(self):
        for half in range(2):
            second = self.spot(half)[1]
            self.arrive(self.got1, self.recv1, half, RAW)
            for h in range(2):
                mine = self.group(half, self.spot(half)[0], h)
                one, two = self.got1.at[half, h, MERGED], self.got1.at[half, 1 - h, RAW]

                @pl.loop(0, self.nf * (SIDE - 1))
                def _(i):
                    f, j = i // (SIDE - 1), (second + 1 + i % (SIDE - 1)) % SIDE
                    total = mine[f, j].astype(jnp.float32) + one[f, j].astype(jnp.float32)
                    mine[f, j] = (total + two[f, j].astype(jnp.float32)).astype(BF16)

            for way in range(2):
                self.hop2(half, way, FAR)
            for way in range(2):
                self.hop2(half, way, RAW)

    def merge2(self):
        for half, way in self.both:
            if way == 0:
                self.arrive(self.got2, self.recv2, half, FAR)
            mine = self.single(half, self.step(self.spot(half)[1], way), way)
            got = self.got2.at[half, way, FAR]
            for f in range(self.nf):
                mine[f] = (mine[f].astype(jnp.float32) + got[f].astype(jnp.float32)).astype(BF16)
            self.hop2(half, way, MERGED)

    def close(self, summed):
        for half in range(2):
            second = self.spot(half)[1]
            self.arrive(self.got2, self.recv2, half, RAW)
            for h in range(2):
                mine = self.single(half, second, h)
                for f in range(self.nf):
                    total = mine[f].astype(jnp.float32)
                    total = total + self.got1[half, h, MERGED, f, second].astype(jnp.float32)
                    total = total + self.got1[half, 1 - h, RAW, f, second].astype(jnp.float32)
                    total = total + self.got2[half, h, MERGED, f].astype(jnp.float32)
                    total = total + self.got2[half, 1 - h, RAW, f].astype(jnp.float32)
                    summed[self.f0 + f, self.lines(half, h)] = total.astype(BF16)


def kernel(x, values_hbm, rows_hbm, cols_hbm, tile_count, w_first_hbm, w_second_hbm, out, *scratch):
    scratch = list(scratch)

    def take(number):
        taken = scratch[:number]
        del scratch[:number]
        return taken

    values, runs, part, summed, staged, plan, plan_smem, tile_rows, tile_cols, w_first, w_second = take(11)
    values_sem, x_sem, plan_sem, out_sem, small_sem, spread_send, share_recv, sum_send = take(8)
    panels = [take(2), take(2)]
    row, col = lax.axis_index("row"), lax.axis_index("col")
    spreads = [
        [
            [
                Spread(unit, panels[layer][f], take(1) + [spread_send, share_recv.at[layer, f]], row, col)
                for unit in SPREADS[layer]
            ]
            for f in range(2)
        ]
        for layer in range(2)
    ]
    sums = [
        [Sum(unit, part, *take(2), take(2) + [sum_send.at[layer]], row, col) for unit in UNITS[layer]]
        for layer in range(2)
    ]

    first_spread = spreads[0][0][0]
    first_sum = sums[0][0]
    partners = [(step, col) for step in first_spread.steps] + [(first_spread.mate, col)]
    for half, way in Sum.both:
        first, second = first_sum.spot(half)
        partners.append((row, first_sum.place(half, first_sum.step(first, way), second)))
    barrier = pltpu.get_barrier_semaphore()
    for to_row, to_col in partners:
        pl.semaphore_signal(barrier, inc=1, device_id=(to_row, to_col), device_id_type=MESH)

    loads = [
        pltpu.make_async_copy(
            x.at[:, :, pl.ds(f * WIDE, WIDE)], panels[0][f].at[pl.ds(row * BLOCK_TILES, BLOCK_TILES)], x_sem.at[f]
        )
        for f in range(2)
    ]
    small = [
        pltpu.make_async_copy(source, target, small_sem.at[i])
        for i, (source, target) in enumerate(
            ((rows_hbm, tile_rows), (cols_hbm, tile_cols), (w_first_hbm, w_first), (w_second_hbm, w_second))
        )
    ]
    for copy in [loads[0]] + small[:2] + [loads[1]] + small[2:]:
        copy.start()
    values_load = pltpu.make_async_copy(values_hbm.at[0, 0], values, values_sem)
    values_load.start()
    pl.semaphore_wait(barrier, len(partners))
    loads[0].wait()
    spreads[0][0][0].own()
    for copy in small:
        copy.wait()

    lane = lax.broadcasted_iota(jnp.int32, (1, SLOTS), 1)
    key = jnp.where(lane < tile_count[0, 0], tile_rows[...] * 64 + tile_cols[...], lane + 8192)
    across = jnp.broadcast_to(key.astype(jnp.float32), (SLOTS, SLOTS))
    down = jnp.transpose(across)
    rank = jnp.sum(jnp.where(across < down, 1.0, 0.0), axis=1, keepdims=True)
    lanes = lax.broadcasted_iota(jnp.int32, (SLOTS, SLOTS), 1).astype(jnp.float32)
    slots = lax.broadcasted_iota(jnp.int32, (SLOTS, SLOTS), 0).astype(jnp.float32)

    def pick(condition, what):
        return jnp.sum(jnp.where(condition, what, 0.0), axis=0, keepdims=True).astype(jnp.int32)

    order = pick(rank == lanes, slots)
    ordered = pick(rank == lanes, down)
    before = pick(rank == lanes - 1.0, down)
    ends = pick(down < (lanes + 1.0) * 64.0, 1.0)
    starts = pick(down < lanes * 64.0, 1.0)
    same = jnp.where(jnp.right_shift(ordered, 6) == jnp.right_shift(before, 6), 1, 0)
    run_of = jnp.where(ends == starts, SLOTS, ends - 1)
    rest = jnp.zeros((4, SLOTS), jnp.int32)
    plan[...] = jnp.concatenate([order, jnp.bitwise_and(ordered, 63), run_of, same, rest], axis=0)
    for f in range(2):
        runs[f, SLOTS] = jnp.zeros((TILE, WIDE), BF16)
    plan_copy = pltpu.make_async_copy(plan, plan_smem, plan_sem)
    plan_copy.start()

    def multiply(panel, f, first, last, total):
        for at in range(first, last):
            slot = jnp.clip(plan_smem[0, at], 0, SLOTS - 1)
            column = jnp.clip(plan_smem[1, at], 0, 63)
            keep = jnp.where(plan_smem[3, at] == 1, 1.0, 0.0)
            total = total * keep + jnp.dot(values[slot], panel[column], preferred_element_type=jnp.float32)
            runs[f, at] = total.astype(BF16)
        return total

    empty = jnp.zeros((TILE, WIDE), jnp.float32)

    def fill(unit, half, first):
        tiles = unit.rows // 2 // TILE
        base = unit.r0 // TILE + half * tiles

        @pl.loop(0, SIDE, unroll=SIDE if tiles == 1 else 1)
        def _(second):
            up, across = (second, first) if half == 0 else (first, second)
            for t in range(base, base + tiles):
                run = jnp.clip(plan_smem[2, (up * SIDE + across) * BLOCK_TILES + t], 0, SLOTS)
                for f in range(unit.f0, unit.f0 + unit.nf):
                    part[f, up, across, pl.ds(t * TILE, TILE)] = runs[f, run]

    def weigh(unit, w, store):
        @pl.loop(0, unit.rows // TILE, unroll=unit.rows // TILE)
        def _(i):
            t = unit.r0 // TILE + i
            lines = pl.ds(pl.multiple_of(t * TILE, TILE), TILE)
            both = jnp.concatenate([summed[0, lines], summed[1, lines]], axis=1)
            product = jnp.dot(both, w[...], preferred_element_type=jnp.float32)
            store(t, jnp.maximum(product, 0.0).astype(BF16))

    def keep_hidden(t, block):
        for f in range(2):
            panels[1][f][row * BLOCK_TILES + t] = block[:, f * WIDE : (f + 1) * WIDE]

    def write(t):
        lines = pl.ds(pl.multiple_of(t * TILE, TILE), TILE)
        return pltpu.make_async_copy(staged.at[lines], out.at[lines], out_sem)

    def keep_output(t, block):
        staged[pl.ds(pl.multiple_of(t * TILE, TILE), TILE)] = block
        write(t).start()

    def shared(layer, f):
        await_bytes(panels[layer][f].at[pl.ds(0, 32)], share_recv.at[layer, f])

    (a,), (b,) = spreads[0]
    a0, a1, b0, b1, b2, b3 = sums[0]
    (g0, g1, g2, g3), (h0, h1, h2, h3) = spreads[1]
    d, e0, e1 = sums[1]
    a.onward(0)
    loads[1].wait()
    b.own()
    a.onward(1)
    a.onward(2)
    shared(0, 0)
    plan_copy.wait()
    values_load.wait()
    multiply(panels[0][0], 0, 0, 256, empty)
    a0.open(fill)
    b.onward(0)
    b.onward(1)
    a0.merge1()
    b.onward(2)
    shared(0, 1)
    a1.open(fill)
    multiply(panels[0][1], 1, 0, 256, empty)
    b1.open(fill)
    a0.turn()
    b0.open(fill)
    b1.merge1()
    b0.merge1()
    b2.open(fill)
    b0.turn()
    a0.merge2()
    a1.merge1()
    b0.merge2()
    b1.turn()
    a0.close(summed)
    b3.open(fill)
    b0.close(summed)
    b1.merge2()
    weigh(b0, w_first, keep_hidden)
    h0.own()
    b2.merge1()
    b3.merge1()
    a1.turn()
    g0.own()
    b1.close(summed)
    weigh(b1, w_first, keep_hidden)
    g1.own()
    b2.turn()
    h1.own()
    b3.turn()
    a1.merge2()
    g0.onward(0)
    b2.merge2()
    b3.merge2()
    h1.onward(0)
    h1.onward(1)
    g1.onward(0)
    a1.close(summed)
    b2.close(summed)
    weigh(b2, w_first, keep_hidden)
    g0.onward(1)
    g1.onward(1)
    g2.own()
    b3.close(summed)
    weigh(b3, w_first, keep_hidden)
    g3.own()
    h2.own()
    g2.onward(0)
    g3.onward(0)
    h3.own()
    h0.onward(0)
    g1.onward(2)
    g2.onward(1)
    g0.onward(2)
    g3.onward(1)
    g2.onward(2)
    h1.onward(2)
    h0.onward(1)
    h2.onward(0)
    g3.onward(2)
    h3.onward(0)
    h2.onward(1)
    shared(1, 0)
    await_bytes(values.at[pl.ds(0, 240)], sum_send.at[0])

    multiply(panels[1][0], 0, 0, 256, empty)
    h2.onward(2)
    h0.onward(2)
    h3.onward(1)
    h3.onward(2)
    d.open(fill)
    shared(1, 1)
    total = multiply(panels[1][1], 1, 0, 128, empty)
    d.merge1()
    total = multiply(panels[1][1], 1, 128, 256, total)
    e1.open(fill)
    e0.open(fill)
    e1.merge1()
    e0.merge1()
    d.turn()
    e1.turn()
    e0.turn()
    d.merge2()
    e1.merge2()
    e0.merge2()
    d.close(summed)
    e1.close(summed)
    weigh(e1, w_second, keep_output)
    e0.close(summed)
    weigh(e0, w_second, keep_output)
    await_bytes(values.at[pl.ds(0, 224)], spread_send)
    await_bytes(values.at[pl.ds(0, 240)], sum_send.at[1])
    await_bytes(staged, out_sem)


def both_layers(x, values, rows, cols, count, w_first, w_second):
    smem, hbm = pl.BlockSpec(memory_space=pltpu.SMEM), pl.BlockSpec(memory_space=pl.ANY)
    dma = pltpu.SemaphoreType.DMA
    scratch = [
        pltpu.VMEM((SLOTS, TILE, TILE), BF16),
        pltpu.VMEM((2, SLOTS + 1, TILE, WIDE), BF16),
        pltpu.VMEM((2, SIDE, SIDE, NODES, WIDE), BF16),
        pltpu.VMEM((2, NODES, WIDE), BF16),
        pltpu.VMEM((NODES, F), BF16),
        pltpu.VMEM((8, SLOTS), jnp.int32),
        pltpu.SMEM((8, SLOTS), jnp.int32),
        pltpu.VMEM((1, SLOTS), jnp.int32),
        pltpu.VMEM((1, SLOTS), jnp.int32),
        pltpu.VMEM((F, F), BF16),
        pltpu.VMEM((F, F), BF16),
        dma,
        dma((2,)),
        dma,
        dma,
        dma((4,)),
        dma,
        dma((2, 2)),
        dma((2,)),
    ]
    scratch += [pltpu.VMEM((64, TILE, WIDE), BF16)] * 4
    for layer in range(2):
        for _ in SPREADS[layer] * 2:
            scratch += [dma((3,))]
    for layer in range(2):
        for _, nf, _, rows_of in UNITS[layer]:
            scratch += [
                pltpu.VMEM((2, 2, 3, nf, SIDE, rows_of // 4, WIDE), BF16),
                pltpu.VMEM((2, 2, 3, nf, rows_of // 4, WIDE), BF16),
                dma((2, 2)), dma((2, 2)),
            ]
    return pl.pallas_call(
        kernel,
        out_shape=jax.ShapeDtypeStruct((NODES, F), BF16),
        in_specs=[hbm, hbm, hbm, hbm, smem, hbm, hbm],
        out_specs=hbm,
        scratch_shapes=scratch,
        compiler_params=pltpu.CompilerParams(
            collective_id=0, has_side_effects=True, vmem_limit_bytes=67043328
        ),
        name="layers",
    )(x, values, rows, cols, count, w_first, w_second)


def shards(features, tile_values, tile_rows, tile_cols, tile_count, w_first, w_second):
    return both_layers(
        features.reshape(BLOCK_TILES, TILE, F), tile_values, tile_rows[0], tile_cols[0], tile_count, w_first, w_second
    )


def solution(mesh):
    return jax.shard_map(
        shards,
        mesh=mesh,
        in_specs=(
            P(("row", "col"), None),
            P("row", "col", None, None, None),
            P("row", "col", None),
            P("row", "col", None),
            P("row", "col"),
            P(),
            P(),
        ),
        out_specs=P(("row", "col"), None),
        check_vma=False,
    )
```
